8 devices in a mesh: rep: 1 (over z), y: 2 (over y), x: 4 (over x, core).
Axes of the slice: x: 2, y: 2, z: 1, core: 2. Of those that a mesh axis runs over, the one named last changes fastest.
Arguments:
- hidden: bfloat16 [64, 4096], P('rep', 'y')
- lengths: int32 [64], P('rep')
- k_cache: bfloat16 [2, 64, 128, 32, 128], P(None, ('rep', 'y'), None, 'x')
- v_cache: bfloat16 [2, 64, 128, 32, 128], P(None, ('rep', 'y'), None, 'x')
- rel_table: bfloat16 [2, 128, 32, 128], P(None, None, 'x')
- norm_attn: bfloat16 [2, 4096], P(None, 'y')
- w_q: bfloat16 [2, 4096, 32, 128], P(None, 'y', 'x')
- w_k: bfloat16 [2, 4096, 32, 128], P(None, 'y', 'x')
- w_v: bfloat16 [2, 4096, 32, 128], P(None, 'y', 'x')
- bias_content: bfloat16 [2, 32, 128], P(None, 'x')
- bias_pos: bfloat16 [2, 32, 128], P(None, 'x')
- w_out: bfloat16 [2, 32, 128, 4096], P(None, 'x', None, 'y')
- norm_mlp: bfloat16 [2, 4096], P(None, 'y')
- w_up: bfloat16 [2, 4096, 16384], P(None, 'y', 'x')
- w_down: bfloat16 [2, 16384, 4096], P(None, 'x', 'y')
Outputs:
- output 1: bfloat16 [64, 4096], P('rep', 'y')
- output 2: bfloat16 [2, 64, 128, 32, 128], P(None, ('rep', 'y'), None, 'x')
- output 3: bfloat16 [2, 64, 128, 32, 128], P(None, ('rep', 'y'), None, 'x')
All inputs are finite; a program needn't handle non-finite values.
Results may differ from the reference program's by a relative error of at most 0.0187194.
Values are sent between devices in bfloat16 or wider.
A program may use at most 1 GiB of HBM per device.

```python
import jax
import jax.numpy as jnp
from jax import lax

D_MODEL = 4096
HEADS = 32
HEAD_DIM = 128
FF_DIM = 16384
SEQ_MAX = 128
BATCH_ROWS = 64
LAYERS = 2

LEN_LOW = max(1, SEQ_MAX // 10)


def relative_table(key):
    feat_half = 64
    dist = jnp.arange(SEQ_MAX, dtype=jnp.float32)
    freqs = 10000.0 ** (-jnp.arange(feat_half, dtype=jnp.float32) / feat_half)
    angle = dist[:, None] * freqs[None, :]
    feats = jnp.concatenate([jnp.sin(angle), jnp.cos(angle)], axis=1)
    proj = jax.random.normal(key, (LAYERS, 2 * feat_half, HEADS * HEAD_DIM), jnp.float32) * feat_half ** -0.5
    table = jnp.einsum("tf,lfe->lte", feats, proj)
    return table.reshape(LAYERS, SEQ_MAX, HEADS, HEAD_DIM).astype(jnp.bfloat16)


def setup_inputs(seed: int = 0, part: int = 0) -> dict:
    base_key = jax.random.key(seed)
    shared = jax.random.split(base_key, 11)
    part_keys = jax.random.split(jax.random.fold_in(base_key, part), 4)

    def normal(key, shape, scale):
        return (jax.random.normal(key, shape, jnp.float32) * scale).astype(jnp.bfloat16)

    def gains(key):
        return (1.0 + 0.3 * jax.random.normal(key, (LAYERS, D_MODEL), jnp.float32)).astype(jnp.bfloat16)

    model_scale = D_MODEL ** -0.5
    out_scale = (HEADS * HEAD_DIM) ** -0.5 * (SEQ_MAX / 64) ** 0.5
    proj_shape = (LAYERS, D_MODEL, HEADS, HEAD_DIM)
    cache_shape = (LAYERS, BATCH_ROWS, SEQ_MAX, HEADS, HEAD_DIM)
    lengths = jax.random.randint(part_keys[3], (BATCH_ROWS,), LEN_LOW, SEQ_MAX, dtype=jnp.int32)
    lengths = lengths.at[0].set(SEQ_MAX - 1).at[1].set(LEN_LOW)
    return {
        "hidden": normal(part_keys[0], (BATCH_ROWS, D_MODEL), 1.0),
        "lengths": lengths,
        "k_cache": normal(part_keys[1], cache_shape, 1.0),
        "v_cache": normal(part_keys[2], cache_shape, 1.0),
        "rel_table": relative_table(shared[0]),
        "norm_attn": gains(shared[1]),
        "w_q": normal(shared[2], proj_shape, model_scale),
        "w_k": normal(shared[3], proj_shape, model_scale),
        "w_v": normal(shared[4], proj_shape, model_scale),
        "bias_content": normal(shared[5], (LAYERS, HEADS, HEAD_DIM), 0.5),
        "bias_pos": normal(shared[6], (LAYERS, HEADS, HEAD_DIM), 0.5),
        "w_out": normal(shared[7], (LAYERS, HEADS, HEAD_DIM, D_MODEL), out_scale),
        "norm_mlp": gains(shared[8]),
        "w_up": normal(shared[9], (LAYERS, D_MODEL, FF_DIM), model_scale),
        "w_down": normal(shared[10], (LAYERS, FF_DIM, D_MODEL), FF_DIM ** -0.5),
    }


def rms_norm(values, gain):
    wide = values.astype(jnp.float32)
    inv_rms = lax.rsqrt(jnp.mean(wide * wide, axis=-1, keepdims=True) + 1e-6)
    return (wide * inv_rms * gain.astype(jnp.float32)).astype(jnp.bfloat16)


def project(normed, weight):
    flat = jnp.dot(normed, weight.reshape(D_MODEL, HEADS * HEAD_DIM), preferred_element_type=jnp.float32)
    return flat.reshape(BATCH_ROWS, HEADS, HEAD_DIM).astype(jnp.bfloat16)


def reference(hidden, lengths, k_cache, v_cache, rel_table, norm_attn, w_q, w_k, w_v, bias_content, bias_pos, w_out, norm_mlp, w_up, w_down):
    positions = jnp.arange(SEQ_MAX)
    row_ids = jnp.arange(BATCH_ROWS)

    def layer_step(state, layer_args):
        (k_layer, v_layer, rel_layer, gain_attn, wq_layer, wk_layer, wv_layer,
         content_bias, pos_bias, wout_layer, gain_mlp, wup_layer, wdown_layer) = layer_args
        normed = rms_norm(state, gain_attn)
        q_new = project(normed, wq_layer)
        k_new = project(normed, wk_layer)
        v_new = project(normed, wv_layer)
        k_upd = k_layer.at[row_ids, lengths].set(k_new)
        v_upd = v_layer.at[row_ids, lengths].set(v_new)
        rel_wide = rel_layer.astype(jnp.float32)
        cbias_wide = content_bias.astype(jnp.float32)
        pbias_wide = pos_bias.astype(jnp.float32)

        def attend_row(row_args):
            q_row, k_rows, v_rows, length = row_args
            q_wide = q_row.astype(jnp.float32)
            q_content = (q_wide + cbias_wide).astype(jnp.bfloat16).astype(jnp.float32)
            q_pos = (q_wide + pbias_wide).astype(jnp.bfloat16).astype(jnp.float32)
            rel_rows = jnp.take(rel_wide, jnp.maximum(length - positions, 0), axis=0)
            scores = jnp.einsum("he,she->hs", q_content, k_rows.astype(jnp.float32))
            scores = scores + jnp.einsum("he,she->hs", q_pos, rel_rows)
            scores = jnp.where(positions[None, :] <= length, scores * HEAD_DIM ** -0.5, -1e30)
            attn_prob = jax.nn.softmax(scores, axis=-1).astype(jnp.bfloat16).astype(jnp.float32)
            return jnp.einsum("hs,she->he", attn_prob, v_rows.astype(jnp.float32)).astype(jnp.bfloat16)

        context = lax.map(attend_row, (q_new, k_upd, v_upd, lengths))
        attn_out = jnp.dot(context.reshape(BATCH_ROWS, HEADS * HEAD_DIM), wout_layer.reshape(HEADS * HEAD_DIM, D_MODEL), preferred_element_type=jnp.float32)
        state = (state.astype(jnp.float32) + attn_out).astype(jnp.bfloat16)
        normed = rms_norm(state, gain_mlp)
        up_proj = jnp.dot(normed, wup_layer, preferred_element_type=jnp.float32).astype(jnp.bfloat16)
        activated = jax.nn.gelu(up_proj.astype(jnp.float32), approximate=True).astype(jnp.bfloat16)
        down_out = jnp.dot(activated, wdown_layer, preferred_element_type=jnp.float32)
        state = (state.astype(jnp.float32) + down_out).astype(jnp.bfloat16)
        return state, (k_upd, v_upd)

    final, (k_all, v_all) = lax.scan(layer_step, hidden, (k_cache, v_cache, rel_table, norm_attn, w_q, w_k, w_v, bias_content, bias_pos, w_out, norm_mlp, w_up, w_down))
    return final, k_all, v_all
```

```python
import functools
import jax
import jax.numpy as jnp
from jax import lax
from jax.experimental import pallas as pl
from jax.experimental.pallas import tpu as pltpu
from jax.sharding import PartitionSpec as P

BF = jnp.bfloat16
F32 = jnp.float32

EPS = 1e-6


def sharded_norm(hidden, gain, d_total):
    hidden_wide = hidden.astype(jnp.float32)
    sum_sq = lax.psum(jnp.sum(hidden_wide * hidden_wide, axis=1, keepdims=True), "y")
    inv_rms = lax.rsqrt(sum_sq / d_total + EPS)
    return (hidden_wide * inv_rms * gain.astype(jnp.float32)).astype(jnp.bfloat16)


def attn_body(layer, group, len_ref, q_ref, kn_ref, vn_ref, rel_ref, u_ref, w_ref, kc, vc, *rest):
    ctx_ref, ko, vo, kbuf, vbuf, rext, rsem, wsem = rest[-8:]
    rows, seq, heads, hd = kbuf.shape
    y = lax.axis_index("y")
    n_grp = rows // group
    span = seq * heads

    def load(i):
        sl = pl.ds(i * group, group)
        return (pltpu.make_async_copy(kc.at[layer, sl], kbuf.at[sl], rsem.at[0, i]),
                pltpu.make_async_copy(vc.at[layer, sl], vbuf.at[sl], rsem.at[1, i]))

    def save(i):
        sl = pl.ds(i * group, group)
        return (pltpu.make_async_copy(kbuf.at[sl], ko.at[layer, sl], wsem.at[0, i]),
                pltpu.make_async_copy(vbuf.at[sl], vo.at[layer, sl], wsem.at[1, i]))

    @pl.loop(0, n_grp)
    def _(i):
        for c in load(i):
            c.start()

    @pl.loop(0, seq)
    def _(t):
        rext[seq - 1 - t] = rel_ref[layer, t]
        rext[seq + t] = jnp.zeros((heads, hd), BF)

    col = lax.broadcasted_iota(jnp.int32, (heads, span), 1)
    row = lax.broadcasted_iota(jnp.int32, (heads, span), 0)
    own = (col % heads) == row
    pos = col // heads
    scale = hd ** -0.5

    @pl.loop(0, n_grp)
    def _(i):
        for c in load(i):
            c.wait()
        outs = []
        for g in range(group):
            b = i * group + g
            ln = len_ref[y * rows + b]
            kbuf[b, ln] = kn_ref[b]
            vbuf[b, ln] = vn_ref[b]
        for g in range(group):
            b = i * group + g
            ln = len_ref[y * rows + b]
            qw = q_ref[b].astype(F32)
            a = (qw + u_ref[layer].astype(F32)).astype(BF)
            c = (qw + w_ref[layer].astype(F32)).astype(BF)
            lhs = jnp.concatenate([a, c], axis=1)
            kk = kbuf[b].reshape(span, hd)
            rr = rext[pl.ds(seq - 1 - ln, seq)].reshape(span, hd)
            rhs = jnp.concatenate([kk, rr], axis=1)
            s = lax.dot_general(lhs, rhs, (((1,), (1,)), ((), ())), preferred_element_type=F32)
            s = jnp.where(own & (pos <= ln), s * scale, -1e30)
            m = jnp.max(s, axis=1, keepdims=True)
            e = jnp.exp(s - m)
            p = (e / jnp.sum(e, axis=1, keepdims=True)).astype(BF)
            o = jnp.dot(p, vbuf[b].reshape(span, hd), preferred_element_type=F32)
            ctx_ref[b] = o.astype(BF)
        for c in save(i):
            c.start()

    @pl.loop(0, n_grp)
    def _(i):
        for c in save(i):
            c.wait()


def attend_cache(layer, lengths, q, kn, vn, rel, u, w, kc, vc, prev, group=4):
    rows, seq, heads, hd = kc.shape[1:]
    any_ = pl.BlockSpec(memory_space=pl.ANY)
    vm = pl.BlockSpec(memory_space=pltpu.VMEM)
    n_grp = rows // group
    ins = [lengths, q, kn, vn, rel, u, w, kc, vc]
    specs = [pl.BlockSpec(memory_space=pltpu.SMEM), vm, vm, vm,
             vm, vm, vm, any_, any_]
    alias = {}
    if prev is not None:
        ins += list(prev)
        specs += [any_, any_]
        alias = {9: 1, 10: 2}
    return pl.pallas_call(
        functools.partial(attn_body, layer, group),
        out_shape=(jax.ShapeDtypeStruct((rows, heads, hd), BF), jax.ShapeDtypeStruct(kc.shape, BF), jax.ShapeDtypeStruct(vc.shape, BF)),
        in_specs=specs,
        out_specs=(vm, any_, any_),
        input_output_aliases=alias,
        scratch_shapes=[pltpu.VMEM((rows, seq, heads, hd), BF), pltpu.VMEM((rows, seq, heads, hd), BF),
                        pltpu.VMEM((2 * seq, heads, hd), BF), pltpu.SemaphoreType.DMA((2, n_grp)), pltpu.SemaphoreType.DMA((2, n_grp))],
        compiler_params=pltpu.CompilerParams(vmem_limit_bytes=40 << 20),
        cost_estimate=pl.CostEstimate(flops=2 * 2 * rows * heads * span_of(seq, heads) * hd, bytes_accessed=4 * rows * seq * heads * hd * 2, transcendentals=rows * heads * seq),
        name=f"attend_{layer}",
    )(*ins)


def span_of(seq, heads):
    return seq * heads


def solution(mesh):
    y_size = mesh.shape["y"]
    cache_spec = P(None, ("rep", "y"), None, "x", None)
    row_spec = P("rep", "y")
    proj_spec = P(None, "y", "x", None)
    head_spec = P(None, "x", None)
    in_specs = (row_spec, P("rep"), cache_spec, cache_spec, P(None, None, "x", None), P(None, "y"),
                proj_spec, proj_spec, proj_spec, head_spec, head_spec, P(None, "x", None, "y"),
                P(None, "y"), P(None, "y", "x"), P(None, "x", "y"))
    out_specs = (row_spec, cache_spec, cache_spec)

    def local_step(hidden, lengths, k_cache, v_cache, rel_table, norm_attn, w_q, w_k, w_v, bias_content, bias_pos, w_out, norm_mlp, w_up, w_down):
        rows_local = k_cache.shape[1]
        row_start = lax.axis_index("y") * rows_local
        len_local = lax.dynamic_slice_in_dim(lengths, row_start, rows_local)
        d_total = hidden.shape[1] * y_size
        prev = None
        for layer in range(k_cache.shape[0]):
            normed = sharded_norm(hidden, norm_attn[layer], d_total)
            q_part = jnp.einsum("bd,dhe->bhe", normed, w_q[layer], preferred_element_type=jnp.float32).astype(jnp.bfloat16)
            k_part = jnp.einsum("bd,dhe->bhe", normed, w_k[layer], preferred_element_type=jnp.float32).astype(jnp.bfloat16)
            v_part = jnp.einsum("bd,dhe->bhe", normed, w_v[layer], preferred_element_type=jnp.float32).astype(jnp.bfloat16)
            q_full, k_full, v_full = lax.psum((q_part, k_part, v_part), "y")
            q_rows = lax.dynamic_slice_in_dim(q_full, row_start, rows_local)
            k_rows = lax.dynamic_slice_in_dim(k_full, row_start, rows_local)
            v_rows = lax.dynamic_slice_in_dim(v_full, row_start, rows_local)
            context, k_out, v_out = attend_cache(layer, lengths, q_rows, k_rows, v_rows, rel_table, bias_content, bias_pos, k_cache, v_cache, prev)
            prev = (k_out, v_out)
            context_all = lax.all_gather(context, "y", axis=0, tiled=True)
            attn_part = jnp.einsum("bhe,hed->bd", context_all, w_out[layer], preferred_element_type=jnp.float32).astype(jnp.bfloat16)
            attn_out = lax.psum(attn_part, "x")
            hidden = (hidden.astype(jnp.float32) + attn_out.astype(jnp.float32)).astype(jnp.bfloat16)
            normed = sharded_norm(hidden, norm_mlp[layer], d_total)
            up_part = jnp.dot(normed, w_up[layer], preferred_element_type=jnp.float32).astype(jnp.bfloat16)
            up_proj = lax.psum(up_part, "y")
            activated = jax.nn.gelu(up_proj.astype(jnp.float32), approximate=True).astype(jnp.bfloat16)
            down_part = jnp.dot(activated, w_down[layer], preferred_element_type=jnp.float32).astype(jnp.bfloat16)
            down_out = lax.psum(down_part, "x")
            hidden = (hidden.astype(jnp.float32) + down_out.astype(jnp.float32)).astype(jnp.bfloat16)
        return hidden, prev[0], prev[1]

    return jax.shard_map(local_step, mesh=mesh, in_specs=in_specs, out_specs=out_specs, check_vma=False)
```

```python
import functools
import jax
import jax.numpy as jnp
from jax import lax
from jax.experimental import pallas as pl
from jax.experimental.pallas import tpu as pltpu
from jax.sharding import PartitionSpec as P

BF = jnp.bfloat16
F32 = jnp.float32

def attn_body(layer, group, len_ref, q_ref, kn_ref, vn_ref, rel_ref, u_ref, w_ref, kc, vc, *rest):
    ctx_ref, ko, vo, kbuf, vbuf, rext, rsem, wsem = rest[-8:]
    rows, seq, heads, hd = kbuf.shape
    y = lax.axis_index("y")
    n_grp = rows // group
    span = seq * heads

    def load(i):
        sl = pl.ds(i * group, group)
        return (pltpu.make_async_copy(kc.at[layer, sl], kbuf.at[sl], rsem.at[0, i]),
                pltpu.make_async_copy(vc.at[layer, sl], vbuf.at[sl], rsem.at[1, i]))

    def save(i):
        sl = pl.ds(i * group, group)
        return (pltpu.make_async_copy(kbuf.at[sl], ko.at[layer, sl], wsem.at[0, i]),
                pltpu.make_async_copy(vbuf.at[sl], vo.at[layer, sl], wsem.at[1, i]))

    @pl.loop(0, n_grp)
    def _(i):
        for c in load(i):
            c.start()

    @pl.loop(0, seq)
    def _(t):
        rext[seq - 1 - t] = rel_ref[layer, t]
        rext[seq + t] = jnp.zeros((heads, hd), BF)

    col = lax.broadcasted_iota(jnp.int32, (heads, span), 1)
    row = lax.broadcasted_iota(jnp.int32, (heads, span), 0)
    own = (col % heads) == row
    pos = col // heads
    scale = hd ** -0.5

    @pl.loop(0, n_grp)
    def _(i):
        for c in load(i):
            c.wait()
        outs = []
        for g in range(group):
            b = i * group + g
            ln = len_ref[y * rows + b]
            kbuf[b, ln] = kn_ref[b].astype(BF)
            vbuf[b, ln] = vn_ref[b].astype(BF)
        for g in range(group):
            b = i * group + g
            ln = len_ref[y * rows + b]
            qw = q_ref[b].astype(F32)
            a = (qw + u_ref[layer].astype(F32)).astype(BF)
            c = (qw + w_ref[layer].astype(F32)).astype(BF)
            lhs = jnp.concatenate([a, c], axis=1)
            kk = kbuf[b].reshape(span, hd)
            rr = rext[pl.ds(seq - 1 - ln, seq)].reshape(span, hd)
            rhs = jnp.concatenate([kk, rr], axis=1)
            s = lax.dot_general(lhs, rhs, (((1,), (1,)), ((), ())), preferred_element_type=F32)
            s = jnp.where(own & (pos <= ln), s * scale, -1e30)
            m = jnp.max(s, axis=1, keepdims=True)
            e = jnp.exp(s - m)
            p = (e / jnp.sum(e, axis=1, keepdims=True)).astype(BF)
            o = jnp.dot(p, vbuf[b].reshape(span, hd), preferred_element_type=F32)
            ctx_ref[b] = o.astype(BF).astype(F32)
        for c in save(i):
            c.start()

    @pl.loop(0, n_grp)
    def _(i):
        for c in save(i):
            c.wait()


def attend_cache(layer, lengths, q, kn, vn, rel, u, w, kc, vc, prev, group=4):
    rows, seq, heads, hd = kc.shape[1:]
    any_ = pl.BlockSpec(memory_space=pl.ANY)
    vm = pl.BlockSpec(memory_space=pltpu.VMEM)
    n_grp = rows // group
    ins = [lengths, q, kn, vn, rel, u, w, kc, vc]
    specs = [pl.BlockSpec(memory_space=pltpu.SMEM), vm, vm, vm,
             vm, vm, vm, any_, any_]
    alias = {}
    if prev is not None:
        ins += list(prev)
        specs += [any_, any_]
        alias = {9: 1, 10: 2}
    return pl.pallas_call(
        functools.partial(attn_body, layer, group),
        out_shape=(jax.ShapeDtypeStruct((rows, heads, hd), F32), jax.ShapeDtypeStruct(kc.shape, BF), jax.ShapeDtypeStruct(vc.shape, BF)),
        in_specs=specs,
        out_specs=(vm, any_, any_),
        input_output_aliases=alias,
        scratch_shapes=[pltpu.VMEM((rows, seq, heads, hd), BF), pltpu.VMEM((rows, seq, heads, hd), BF),
                        pltpu.VMEM((2 * seq, heads, hd), BF), pltpu.SemaphoreType.DMA((2, n_grp)), pltpu.SemaphoreType.DMA((2, n_grp))],
        compiler_params=pltpu.CompilerParams(vmem_limit_bytes=40 << 20),
        cost_estimate=pl.CostEstimate(flops=2 * 2 * rows * heads * span_of(seq, heads) * hd, bytes_accessed=4 * rows * seq * heads * hd * 2, transcendentals=rows * heads * seq),
        name=f"attend_{layer}",
    )(*ins)


def span_of(seq, heads):
    return seq * heads


MESH = pl.DeviceIdType.MESH
EPS = 1e-6
UP_CHUNK = 512
DIM_NT = (((1,), (1,)), ((), ()))


def rows_to_cols(col):
    square = jnp.concatenate([col] * (128 // col.shape[0]), axis=0)
    return jnp.broadcast_to(jnp.sum(square.T, axis=0, keepdims=True), (8, 128))


def cols_to_rows(row, n):
    return jnp.broadcast_to(row[0:1], (128, 128)).T[:n, 0:1]


def stage_body(pre, qkv, layer, names, *refs):
    r = dict(zip(names, refs))
    batch, width = r["hidden"].shape
    half = width // 2
    rows = batch // 2
    x = lax.axis_index("x")
    y = lax.axis_index("y")
    y_dev = {"y": 1 - y}
    core = x % 2
    pair_dev = {"x": x + 1 - 2 * core}
    chip_dev = {"x": (x + 2) % 4}
    qkv_layer = layer + 1 if pre else layer

    def remote(src, dst, sems, idx, dev):
        return pltpu.make_async_remote_copy(src, dst, r[sems].at[0, idx], r[sems].at[1, idx], device_id=dev, device_id_type=MESH)

    def wo_copy(i):
        n = r["wo"].shape[0] // 4
        return pltpu.make_async_copy(r["w_out"].at[layer, pl.ds(i * n, n)], r["wo"].at[pl.ds(i * n, n)], r["wo_sem"].at[i])

    def up_copy(i):
        cols = pl.ds(pl.multiple_of(i * UP_CHUNK, UP_CHUNK), UP_CHUNK)
        return pltpu.make_async_copy(r["w_up"].at[layer, :, cols], r["wup"].at[:, cols], r["wup_sem"].at[i])

    def down_copy(i):
        sl = pl.ds(i * UP_CHUNK, UP_CHUNK)
        return pltpu.make_async_copy(r["w_down"].at[layer, sl], r["wdn"].at[sl], r["wdn_sem"].at[i])

    def qkv_copy(m, i):
        sl = pl.ds(i * 512, 512)
        return pltpu.make_async_copy(r[("w_q", "w_k", "w_v")[m]].at[qkv_layer, sl], r["wqkv"].at[m, sl], r["wqkv_sem"].at[m, i])

    k_chunks = width // 512

    def start_qkv():
        for m in range(3):
            for i in range(k_chunks):
                qkv_copy(m, i).start()

    if pre:
        n_up = r["wup"].shape[1] // UP_CHUNK
        for i in range(4):
            wo_copy(i).start()

        @pl.loop(0, n_up)
        def _(i):
            up_copy(i).start()
    else:
        start_qkv()

    barrier = pltpu.get_barrier_semaphore()
    greet = [y_dev, pair_dev, chip_dev] if pre else [y_dev]
    for dev in greet:
        pl.semaphore_signal(barrier, inc=1, device_id=dev, device_id_type=MESH)
    pl.semaphore_wait(barrier, len(greet))

    def norm(x_ref, gain_ref, gain_layer, slot):
        wide = x_ref[...].astype(F32)
        sq = wide * wide
        part = sq[:, 0:128]
        for j in range(1, width // 128):
            part = part + sq[:, j * 128:(j + 1) * 128]
        r["ss_send"][slot] = rows_to_cols(part)
        cp = remote(r["ss_send"].at[slot], r["ss_recv"].at[slot], "ss_sem", slot, y_dev)
        cp.start()
        cp.wait()
        total = cols_to_rows(r["ss_send"][slot] + r["ss_recv"][slot], batch)
        inv = lax.rsqrt(total / (2 * width) + EPS)
        gain = gain_ref[pl.ds(gain_layer, 1)].astype(F32)
        r["h"][...] = (x_ref[...].astype(F32) * inv * gain).astype(BF)

    own = pl.ds(pl.multiple_of(core * half, half), half)
    other = pl.ds(pl.multiple_of((1 - core) * half, half), half)

    def reduce_x(slot, part_of, x_ref, out_ref):
        r["pair_send"][slot] = part_of(other).astype(BF)
        to_pair = remote(r["pair_send"].at[slot], r["pair_recv"].at[slot], "pair_sem", slot, pair_dev)
        to_pair.start()
        r["part"][...] = part_of(own)
        to_pair.wait()
        r["chip_send"][slot] = (r["part"][...] + r["pair_recv"][slot].astype(F32)).astype(BF)
        to_chip = remote(r["chip_send"].at[slot], r["chip_recv"].at[slot], "chip_sem", slot, chip_dev)
        to_chip.start()
        to_chip.wait()
        total = r["chip_send"][slot].astype(F32) + r["chip_recv"][slot].astype(F32)
        out_ref[:, own] = (x_ref[:, own].astype(F32) + total).astype(BF)
        share = remote(out_ref.at[:, own], out_ref.at[:, own], "share_sem", slot, pair_dev)
        share.start()
        share.wait()

    x_now = r["hidden"]
    if pre:
        mine = pl.ds(pl.multiple_of(y * rows, rows), rows)
        heads, hd = r["ctx"].shape[1:]
        for hh in range(heads):
            r["ctx_all"][mine, hh * hd:(hh + 1) * hd] = r["ctx"][:, hh, :].astype(BF)
        cp = remote(r["ctx_all"].at[mine], r["ctx_all"].at[mine], "ctx_sem", 0, y_dev)
        cp.start()
        for i in range(4):
            wo_copy(i).wait()
        cp.wait()

        def wo_part(cols):
            return jnp.dot(r["ctx_all"][...], r["wo"][:, cols], preferred_element_type=F32)

        reduce_x(0, wo_part, r["hidden"], r["x_mid"])

        @pl.loop(0, n_up)
        def _(i):
            down_copy(i).start()
        if qkv:
            start_qkv()

        norm(r["x_mid"], r["g_mlp"], layer, 0)

        def exchange_up(i):
            cols = pl.ds(pl.multiple_of(i * UP_CHUNK, UP_CHUNK), UP_CHUNK)
            return remote(r["up_send"].at[:, cols], r["up_recv"].at[:, cols], "up_sem", i, y_dev)

        @pl.loop(0, n_up)
        def _(i):
            up_copy(i).wait()
            cols = pl.ds(pl.multiple_of(i * UP_CHUNK, UP_CHUNK), UP_CHUNK)
            r["up_send"][:, cols] = jnp.dot(r["h"][...], r["wup"][:, cols], preferred_element_type=F32).astype(BF)
            exchange_up(i).start()

        def activate(i):
            cols = pl.ds(pl.multiple_of(i * UP_CHUNK, UP_CHUNK), UP_CHUNK)
            exchange_up(i).wait()
            m = (r["up_send"][:, cols].astype(F32) + r["up_recv"][:, cols].astype(F32)).astype(BF)
            r["act"][...] = jax.nn.gelu(m.astype(F32), approximate=True).astype(BF)

        r["acc"][...] = jnp.zeros_like(r["acc"])

        @pl.loop(0, n_up - 1)
        def _(i):
            down_copy(i).wait()
            activate(i)
            sl = pl.ds(pl.multiple_of(i * UP_CHUNK, UP_CHUNK), UP_CHUNK)
            r["acc"][...] += jnp.dot(r["act"][...], r["wdn"][sl, :], preferred_element_type=F32)

        down_copy(n_up - 1).wait()
        activate(n_up - 1)

        def down_part(cols):
            last = jnp.dot(r["act"][...], r["wdn"][pl.ds((n_up - 1) * UP_CHUNK, UP_CHUNK), cols], preferred_element_type=F32)
            return r["acc"][:, cols] + last

        reduce_x(1, down_part, r["x_mid"], r["x_end"])
        r["x_out"][...] = r["x_end"][...]
        x_now = r["x_end"]

    if qkv:
        norm(x_now, r["g_attn"], qkv_layer, 1)
        heads, hd = r["wqkv"].shape[2:]
        mine = pl.ds(pl.multiple_of(y * rows, rows), rows)
        theirs = pl.ds(pl.multiple_of((1 - y) * rows, rows), rows)

        def swap(m):
            return remote(r["qkv_send"].at[m], r["qkv_recv"].at[m], "qkv_sem", m, y_dev)

        for m in range(3):
            for i in range(k_chunks):
                qkv_copy(m, i).wait()
            r["part"][...] = jnp.zeros_like(r["part"])

            @pl.loop(0, k_chunks)
            def _(i):
                sl = pl.ds(pl.multiple_of(i * 512, 512), 512)
                by_head = jnp.swapaxes(r["wqkv"][m, sl], 0, 1)
                flat = jnp.concatenate([by_head[hh] for hh in range(heads)], axis=1)
                r["part"][...] += jnp.dot(r["h"][:, sl], flat, preferred_element_type=F32)

            r["qkv_send"][m] = r["part"][theirs, :].astype(BF)
            swap(m).start()
            r["qkv_own"][m] = r["part"][mine, :].astype(BF)

        for m in range(3):
            swap(m).wait()
            full = (r["qkv_own"][m].astype(F32) + r["qkv_recv"][m].astype(F32)).astype(BF).astype(F32)
            out = r[("q", "k", "v")[m]]
            for hh in range(heads):
                out[:, hh, :] = full[:, hh * hd:(hh + 1) * hd]


def stage(pre, qkv, layer, hidden, ctx, w):
    batch, width = hidden.shape
    heads, hd = w["w_q"].shape[2:]
    rows, half, flat = batch // 2, width // 2, heads * hd
    ff = w["w_up"].shape[2]
    n_up = ff // UP_CHUNK
    vm = pl.BlockSpec(memory_space=pltpu.VMEM)
    any_ = pl.BlockSpec(memory_space=pl.ANY)
    dma = pltpu.SemaphoreType.DMA
    ins = [("hidden", hidden, vm)]
    outs = []
    scratch = [("ss_send", pltpu.VMEM((2, 8, 128), F32)), ("ss_recv", pltpu.VMEM((2, 8, 128), F32)), ("ss_sem", dma((2, 2))),
               ("h", pltpu.VMEM((batch, width), BF)), ("part", pltpu.VMEM((batch, half), F32))]
    if pre:
        ins += [("ctx", ctx, vm), ("g_mlp", w["norm_mlp"], vm), ("w_out", w["w_out"], any_), ("w_up", w["w_up"], any_), ("w_down", w["w_down"], any_)]
        outs += [("x_out", (batch, width), BF)]
        piece = pltpu.VMEM((2, batch, half), BF)
        scratch += [("wo", pltpu.VMEM((flat, width), BF)), ("wo_sem", dma((4,))),
                    ("wup", pltpu.VMEM((width, ff), BF)), ("wup_sem", dma((n_up,))),
                    ("wdn", pltpu.VMEM((ff, width), BF)), ("wdn_sem", dma((n_up,))),
                    ("pair_send", piece), ("pair_recv", piece), ("pair_sem", dma((2, 2))),
                    ("chip_send", piece), ("chip_recv", piece), ("chip_sem", dma((2, 2))), ("share_sem", dma((2, 2))),
                    ("ctx_all", pltpu.VMEM((batch, flat), BF)), ("ctx_sem", dma((2, 1))),
                    ("x_mid", pltpu.VMEM((batch, width), BF)), ("x_end", pltpu.VMEM((batch, width), BF)),
                    ("up_send", pltpu.VMEM((batch, ff), BF)), ("up_recv", pltpu.VMEM((batch, ff), BF)), ("up_sem", dma((2, n_up))),
                    ("act", pltpu.VMEM((batch, UP_CHUNK), BF)), ("acc", pltpu.VMEM((batch, width), F32))]
    if qkv:
        ins += [("g_attn", w["norm_attn"], vm), ("w_q", w["w_q"], any_), ("w_k", w["w_k"], any_), ("w_v", w["w_v"], any_)]
        outs += [(n, (rows, heads, hd), F32) for n in ("q", "k", "v")]
        share = pltpu.VMEM((3, rows, flat), BF)
        scratch += [("wqkv", pltpu.VMEM((3, width, heads, hd), BF)), ("wqkv_sem", dma((3, width // 512))),
                    ("qkv_send", share), ("qkv_recv", share), ("qkv_own", share), ("qkv_sem", dma((2, 3)))]
    names = [n for n, *_ in ins] + [n for n, *_ in outs] + [n for n, _ in scratch]
    return pl.pallas_call(
        functools.partial(stage_body, pre, qkv, layer, names),
        out_shape=tuple(jax.ShapeDtypeStruct(s, d) for _, s, d in outs),
        in_specs=[s for *_, s in ins],
        out_specs=tuple(vm for _ in outs),
        scratch_shapes=[s for _, s in scratch],
        compiler_params=pltpu.CompilerParams(collective_id=(1 if pre else 0) + (2 if qkv else 0), has_side_effects=True,
                                             vmem_limit_bytes=62 << 20),
        name=f"stage_{int(pre)}{int(qkv)}",
    )(*[a for _, a, _ in ins])


def solution(mesh):
    cache_spec = P(None, ("rep", "y"), None, "x", None)
    row_spec = P("rep", "y")
    proj_spec = P(None, "y", "x", None)
    head_spec = P(None, "x", None)
    in_specs = (row_spec, P("rep"), cache_spec, cache_spec, P(None, None, "x", None), P(None, "y"),
                proj_spec, proj_spec, proj_spec, head_spec, head_spec, P(None, "x", None, "y"),
                P(None, "y"), P(None, "y", "x"), P(None, "x", "y"))
    out_specs = (row_spec, cache_spec, cache_spec)

    def local_step(hidden, lengths, k_cache, v_cache, rel_table, norm_attn, w_q, w_k, w_v, bias_content, bias_pos, w_out, norm_mlp, w_up, w_down):
        w = dict(norm_attn=norm_attn, w_q=w_q, w_k=w_k, w_v=w_v, norm_mlp=norm_mlp, w_up=w_up, w_down=w_down,
                 w_out=w_out.reshape(w_out.shape[0], -1, w_out.shape[3]))
        layers = k_cache.shape[0]
        q, k, v = stage(False, True, 0, hidden, None, w)
        prev = None
        for layer in range(layers):
            ctx, *prev = attend_cache(layer, lengths, q, k, v, rel_table, bias_content, bias_pos, k_cache, v_cache, prev)
            if layer + 1 < layers:
                hidden, q, k, v = stage(True, True, layer, hidden, ctx, w)
            else:
                hidden, = stage(True, False, layer, hidden, ctx, w)
        return hidden, prev[0], prev[1]

    return jax.shard_map(local_step, mesh=mesh, in_specs=in_specs, out_specs=out_specs, check_vma=False)
```

```python
import functools
import jax
import jax.numpy as jnp
from jax import lax
from jax.experimental import pallas as pl
from jax.experimental.pallas import tpu as pltpu
from jax.sharding import PartitionSpec as P

BF = jnp.bfloat16
F32 = jnp.float32

def attn_body(layer, group, len_ref, q_hbm, kn_hbm, vn_hbm, rel_hbm, u_hbm, w_hbm, k_in, v_in, *rest):
    ctx_hbm, ko, vo, kbuf, vbuf, q_ref, kn_ref, vn_ref, rel_ref, u_ref, w_ref, ctx_ref, rext, osem, wsem = rest[-15:]
    rows, span, hd = kbuf.shape
    heads = q_ref.shape[1]
    seq = span // heads
    y = lax.axis_index("y")
    n_grp = rows // group
    small = [(rel_hbm.at[layer], rel_ref), (q_hbm, q_ref), (kn_hbm, kn_ref), (vn_hbm, vn_ref), (u_hbm, u_ref), (w_hbm, w_ref)]
    small = [pltpu.make_async_copy(src, dst, osem.at[i]) for i, (src, dst) in enumerate(small)]
    for c in small:
        c.start()

    def save(i):
        sl = pl.ds(i * group, group)
        return (pltpu.make_async_copy(kbuf.at[sl], ko.at[layer, sl], wsem.at[0, i]),
                pltpu.make_async_copy(vbuf.at[sl], vo.at[layer, sl], wsem.at[1, i]),
                pltpu.make_async_copy(ctx_ref.at[sl], ctx_hbm.at[sl], wsem.at[2, i]))

    @pl.loop(0, seq, unroll=4)
    def _(t):
        rext[pl.ds(pl.multiple_of((seq + t) * heads, heads), heads)] = jnp.zeros((heads, hd), BF)

    small[0].wait()

    @pl.loop(0, seq, unroll=4)
    def _(t):
        rext[pl.ds(pl.multiple_of((seq - 1 - t) * heads, heads), heads)] = rel_ref[t]

    col = lax.broadcasted_iota(jnp.int32, (heads, span), 1)
    row = lax.broadcasted_iota(jnp.int32, (heads, span), 0)
    own = (col % heads) == row
    pos = jnp.where(own, col // heads, 1 << 20)
    scale = hd ** -0.5
    for c in small[1:]:
        c.wait()

    @pl.loop(0, n_grp)
    def _(i):
        for g in range(group):
            b = i * group + g
            ln = len_ref[y * rows + b]
            at = pl.ds(pl.multiple_of(ln * heads, heads), heads)
            kbuf[b, at] = kn_ref[b].astype(BF)
            vbuf[b, at] = vn_ref[b].astype(BF)
        score = []
        for g in range(group):
            b = i * group + g
            ln = len_ref[y * rows + b]
            qw = q_ref[b].astype(F32)
            a = (qw + u_ref[layer].astype(F32)).astype(BF)
            c = (qw + w_ref[layer].astype(F32)).astype(BF)
            rr = rext[pl.ds(pl.multiple_of((seq - 1 - ln) * heads, heads), span)]
            lhs = jnp.concatenate([a, c], axis=1)
            rhs = jnp.concatenate([kbuf[b], rr], axis=1)
            s = lax.dot_general(lhs, rhs, (((1,), (1,)), ((), ())), preferred_element_type=F32)
            score.append(jnp.where(pos <= ln, s * scale, -1e30))
        prob = []
        for g in range(group):
            s = score[g]
            m = jnp.max(s, axis=1, keepdims=True)
            e = jnp.exp(s - m)
            prob.append((e / jnp.sum(e, axis=1, keepdims=True)).astype(BF))
        for g in range(group):
            b = i * group + g
            o = jnp.dot(prob[g], vbuf[b], preferred_element_type=F32)
            ctx_ref[b] = o.astype(BF).astype(F32)
        for c in save(i):
            c.start()

    @pl.loop(0, n_grp)
    def _(i):
        for c in save(i):
            c.wait()


def attend_cache(layer, lengths, q, kn, vn, rel, u, w, k_now, v_now, layers, prev, group=8):
    rows, span, hd = k_now.shape
    heads = q.shape[1]
    seq = span // heads
    any_ = pl.BlockSpec(memory_space=pl.ANY)
    vm = pl.BlockSpec(memory_space=pltpu.VMEM)
    n_grp = rows // group
    k_now, v_now = (pltpu.with_memory_space_constraint(c, pltpu.VMEM) for c in (k_now, v_now))
    ins = [lengths, q, kn, vn, rel, u, w, k_now, v_now]
    specs = [pl.BlockSpec(memory_space=pltpu.SMEM)] + [any_] * 6 + [vm, vm]
    alias = {7: 3, 8: 4}
    if prev is not None:
        ins += prev
        specs += [any_, any_]
        alias.update({9: 1, 10: 2})
    cache = jax.ShapeDtypeStruct((layers, rows, span, hd), BF)
    now = jax.ShapeDtypeStruct(k_now.shape, BF)
    rows_f32 = pltpu.VMEM((rows, heads, hd), F32)
    return pl.pallas_call(
        functools.partial(attn_body, layer, group),
        out_shape=(jax.ShapeDtypeStruct((rows, heads, hd), F32), cache, cache, now, now),
        in_specs=specs, out_specs=(any_, any_, any_, vm, vm), input_output_aliases=alias,
        scratch_shapes=[rows_f32, rows_f32, rows_f32, pltpu.VMEM((seq, heads, hd), BF), pltpu.VMEM(u.shape, BF), pltpu.VMEM(w.shape, BF),
                        rows_f32, pltpu.VMEM((2 * seq * heads, hd), BF), pltpu.SemaphoreType.DMA((6,)), pltpu.SemaphoreType.DMA((3, n_grp))],
        compiler_params=pltpu.CompilerParams(vmem_limit_bytes=VMEM_LIMIT),
        name=f"attend_{layer}")(*ins)[:3]


MESH = pl.DeviceIdType.MESH
EPS = 1e-6
UP_CHUNK = 512
RAW_CHUNK = 512
PIECES = 4
VMEM_LIMIT = 46 << 20


def rows_to_cols(col):
    square = jnp.concatenate([col] * (128 // col.shape[0]), axis=0)
    return jnp.broadcast_to(jnp.sum(square.T, axis=0, keepdims=True), (8, 128))


def cols_to_rows(row, n):
    return jnp.broadcast_to(row[0:1], (128, 128)).T[:n, 0:1]


def stage_body(pre, qkv, layer, names, *refs):
    r = dict(zip(names, refs))
    batch, width = r["hidden"].shape
    ops = ["hidden"] + (["ctx", "g_mlp"] if pre else []) + (["g_attn"] if qkv else [])
    operand = {n: pltpu.make_async_copy(r[n], r["v_" + n], r["op_sem"].at[i]) for i, n in enumerate(ops)}
    for n in ops[::-1]:
        operand[n].start()
    result = {}
    half = width // 2
    rows = batch // 2
    x = lax.axis_index("x")
    y = lax.axis_index("y")
    y_dev = {"y": 1 - y}
    core = x % 2
    pair_dev = {"x": x + 1 - 2 * core}
    far_dev = {"x": x + 1 - 2 * core, "y": 1 - y}
    chip_dev = {"x": (x + 2) % 4}
    qkv_layer = layer + 1 if pre else layer

    def remote(src, dst, sems, idx, dev):
        return pltpu.make_async_remote_copy(src, dst, r[sems].at[0, idx], r[sems].at[1, idx], device_id=dev, device_id_type=MESH)

    def wo_copy(i):
        n = r["wo"].shape[0] // 4
        return pltpu.make_async_copy(r["w_out"].at[layer, pl.ds(i * n, n)], r["wo"].at[pl.ds(i * n, n)], r["wo_sem"].at[i])

    def up_copy(i):
        cols = pl.ds(pl.multiple_of(i * UP_CHUNK, UP_CHUNK), UP_CHUNK)
        return pltpu.make_async_copy(r["w_up"].at[layer, :, cols], r["wup"].at[:, cols], r["wup_sem"].at[i])

    def down_copy(i):
        sl = pl.ds(i * UP_CHUNK, UP_CHUNK)
        return pltpu.make_async_copy(r["w_down"].at[layer, sl], r["wdn"].at[sl], r["wdn_sem"].at[i])

    k_chunks = width // RAW_CHUNK

    def cache_copies(i):
        src, dst = (("k_cache", "k_now"), ("v_cache", "v_now"))[i]
        n = r[dst].shape[0] // 4
        return [pltpu.make_async_copy(r[src].at[qkv_layer, pl.ds(j * n, n)], r[dst].at[pl.ds(j * n, n)], r["cache_sem"].at[i, j]) for j in range(4)]

    def raw_copy(m, i):
        sl = pl.ds(i * RAW_CHUNK, RAW_CHUNK)
        return pltpu.make_async_copy(r[("w_q", "w_k", "w_v")[m]].at[qkv_layer, sl], r["wraw"].at[i], r["wraw_sem"].at[i])

    def start_qkv():
        for i in range(k_chunks):
            raw_copy(0, i).start()

    def flatten(m):
        heads, hd = r["wraw"].shape[2:]

        @pl.loop(0, k_chunks)
        def _(i):
            raw_copy(m, i).wait()

            @pl.loop(0, RAW_CHUNK // 256)
            def _(j):
                off = pl.multiple_of(j * 256, 256)
                by_head = jnp.swapaxes(r["wraw"][i, pl.ds(off, 256)], 0, 1)
                sl = pl.ds(pl.multiple_of(i * RAW_CHUNK + off, 256), 256)
                for hh in range(heads):
                    col = m * heads * hd + hh * hd
                    r["wup"][sl, col:col + hd] = by_head[hh]

            if m < 2:
                raw_copy(m + 1, i).start()

        first = 0 if not pre else 2
        if m == first:
            for c in cache_copies(0):
                c.start()
        if m == min(first + 1, 2):
            for c in cache_copies(1):
                c.start()

    if pre:
        n_up = r["wup"].shape[1] // UP_CHUNK
        for i in range(4):
            wo_copy(i).start()

        @pl.loop(0, n_up)
        def _(i):
            up_copy(i).start()
    else:
        start_qkv()

    barrier = pltpu.get_barrier_semaphore()
    greet = [y_dev, pair_dev, chip_dev, far_dev] if pre else [y_dev]
    for dev in greet:
        pl.semaphore_signal(barrier, inc=1, device_id=dev, device_id_type=MESH)
    pl.semaphore_wait(barrier, len(greet))

    def row_sums(wide):
        sq = wide * wide
        part = sq[:, 0:128]
        for j in range(1, wide.shape[1] // 128):
            part = part + sq[:, j * 128:(j + 1) * 128]
        return part

    def sum_copy(slot, j, dev):
        return pltpu.make_async_remote_copy(r["ss_send"].at[slot], r["ss_recv"].at[slot, j], r["ss_sem"].at[0, slot, j], r["ss_sem"].at[1, slot, j],
                                            device_id=dev, device_id_type=MESH)

    def send_sums(slot, part, devs):
        r["ss_send"][slot] = rows_to_cols(part)
        for j, dev in enumerate(devs):
            sum_copy(slot, j, dev).start()

    def normalize(slot, devs, x_ref, gain_ref, gain_layer):
        for j, dev in enumerate(devs):
            sum_copy(slot, j, dev).wait()
        total = r["ss_send"][slot] + r["ss_recv"][slot, 0]
        if len(devs) > 1:
            total = total + (r["ss_recv"][slot, 1] + r["ss_recv"][slot, 2])
        inv = lax.rsqrt(cols_to_rows(total, batch) / (2 * width) + EPS)
        gain = gain_ref[pl.ds(gain_layer, 1)].astype(F32)
        r["h"][...] = (x_ref[...].astype(F32) * inv * gain).astype(BF)

    cells = [pair_dev, y_dev, far_dev]
    step = half // PIECES

    def piece(side, c):
        return pl.ds(pl.multiple_of(side * half + c * step, step), step)

    def reduce_x(slot, part_of, x_ref, out_ref, sums):
        def copy(kind, c):
            here = pl.ds(c * step, step)
            sems = r[kind + "_sem"]
            if kind == "share":
                src = dst = out_ref.at[:, piece(core, c)]
            else:
                src, dst = r[kind + "_send"].at[slot, :, here], r[kind + "_recv"].at[slot, :, here]
            return pltpu.make_async_remote_copy(src, dst, sems.at[0, slot, c], sems.at[1, slot, c],
                                                device_id=chip_dev if kind == "chip" else pair_dev, device_id_type=MESH)

        r["pair_send"][slot] = part_of(pl.ds(pl.multiple_of((1 - core) * half, half), half)).astype(BF)
        for c in range(PIECES):
            copy("pair", c).start()
        r["part"][...] = part_of(pl.ds(pl.multiple_of(core * half, half), half))
        for c in range(PIECES):
            copy("pair", c).wait()
            here = slice(c * step, (c + 1) * step)
            r["chip_send"][slot, :, here] = (r["part"][:, here] + r["pair_recv"][slot, :, here].astype(F32)).astype(BF)
            copy("chip", c).start()
        part = None
        for c in range(PIECES):
            copy("chip", c).wait()
            here = slice(c * step, (c + 1) * step)
            total = r["chip_send"][slot, :, here].astype(F32) + r["chip_recv"][slot, :, here].astype(F32)
            new = (x_ref[:, piece(core, c)].astype(F32) + total).astype(BF)
            out_ref[:, piece(core, c)] = new
            copy("share", c).start()
            if sums:
                add = row_sums(new.astype(F32))
                part = add if part is None else part + add
        if sums:
            send_sums(slot, part, cells)
        for c in range(PIECES):
            copy("share", c).wait()

    x_now = r["v_hidden"]
    if pre:
        operand["ctx"].wait()
        mine = pl.ds(pl.multiple_of(y * rows, rows), rows)
        heads, hd = r["ctx"].shape[1:]
        for hh in range(heads):
            r["ctx_all"][mine, hh * hd:(hh + 1) * hd] = r["v_ctx"][:, hh, :].astype(BF)
        cp = remote(r["ctx_all"].at[mine], r["ctx_all"].at[mine], "ctx_sem", 0, y_dev)
        cp.start()
        for i in range(4):
            wo_copy(i).wait()
        cp.wait()

        def wo_part(cols):
            return jnp.dot(r["ctx_all"][...], r["wo"][:, cols], preferred_element_type=F32)

        operand["hidden"].wait()
        operand["g_mlp"].wait()
        reduce_x(0, wo_part, r["v_hidden"], r["x_mid"], True)

        @pl.loop(0, n_up)
        def _(i):
            down_copy(i).start()
        if qkv:
            start_qkv()

        normalize(0, cells, r["x_mid"], r["v_g_mlp"], layer)

        def exchange_up(i):
            cols = pl.ds(pl.multiple_of(i * UP_CHUNK, UP_CHUNK), UP_CHUNK)
            return remote(r["up_send"].at[:, cols], r["up_recv"].at[:, cols], "up_sem", i, y_dev)

        @pl.loop(0, n_up)
        def _(i):
            up_copy(i).wait()
            cols = pl.ds(pl.multiple_of(i * UP_CHUNK, UP_CHUNK), UP_CHUNK)
            r["up_send"][:, cols] = jnp.dot(r["h"][...], r["wup"][:, cols], preferred_element_type=F32).astype(BF)
            exchange_up(i).start()

        if qkv:
            for m in range(3):
                flatten(m)

        def activate(i):
            cols = pl.ds(pl.multiple_of(i * UP_CHUNK, UP_CHUNK), UP_CHUNK)
            exchange_up(i).wait()
            m = (r["up_send"][:, cols].astype(F32) + r["up_recv"][:, cols].astype(F32)).astype(BF)
            r["act"][...] = jax.nn.gelu(m.astype(F32), approximate=True).astype(BF)

        r["acc"][...] = jnp.zeros_like(r["acc"])

        @pl.loop(0, n_up - 1)
        def _(i):
            down_copy(i).wait()
            activate(i)
            sl = pl.ds(pl.multiple_of(i * UP_CHUNK, UP_CHUNK), UP_CHUNK)
            r["acc"][...] += jnp.dot(r["act"][...], r["wdn"][sl, :], preferred_element_type=F32)

        down_copy(n_up - 1).wait()
        activate(n_up - 1)

        def down_part(cols):
            last = jnp.dot(r["act"][...], r["wdn"][pl.ds((n_up - 1) * UP_CHUNK, UP_CHUNK), cols], preferred_element_type=F32)
            return r["acc"][:, cols] + last

        reduce_x(1, down_part, r["x_mid"], r["x_end"], qkv)
        result["x_out"] = pltpu.make_async_copy(r["x_end"], r["x_out"], r["out_sem"].at[0])
        result["x_out"].start()
        x_now = r["x_end"]

    if qkv:
        heads, hd = r["wraw"].shape[2:]
        operand["g_attn"].wait()
        if pre:
            normalize(1, cells, x_now, r["v_g_attn"], qkv_layer)
        else:
            operand["hidden"].wait()
            send_sums(1, row_sums(x_now[...].astype(F32)), [y_dev])
            flatten(0)
            normalize(1, [y_dev], x_now, r["v_g_attn"], qkv_layer)
        mine = pl.ds(pl.multiple_of(y * rows, rows), rows)
        theirs = pl.ds(pl.multiple_of((1 - y) * rows, rows), rows)

        def swap(m):
            return remote(r["qkv_send"].at[m], r["qkv_recv"].at[m], "qkv_sem", m, y_dev)

        for m in range(3):
            if not pre and m > 0:
                flatten(m)
            for j in range(heads * hd // 256):
                cols = slice(j * 256, (j + 1) * 256)
                lanes = slice(m * heads * hd + j * 256, m * heads * hd + (j + 1) * 256)
                r["part"][:, cols] = jnp.dot(r["h"][...], r["wup"][:, lanes], preferred_element_type=F32)
            r["qkv_send"][m] = r["part"][theirs, :].astype(BF)
            swap(m).start()
            r["qkv_own"][m] = r["part"][mine, :].astype(BF)

        for m in range(3):
            swap(m).wait()
            full = (r["qkv_own"][m].astype(F32) + r["qkv_recv"][m].astype(F32)).astype(BF).astype(F32)
            name = ("q", "k", "v")[m]
            for hh in range(heads):
                r["v_" + name][:, hh, :] = full[:, hh * hd:(hh + 1) * hd]
            result[name] = pltpu.make_async_copy(r["v_" + name], r[name], r["out_sem"].at[m + 1])
            result[name].start()
        for c in cache_copies(0) + cache_copies(1):
            c.wait()
    for c in result.values():
        c.wait()


def stage(pre, qkv, layer, hidden, ctx, w):
    batch, width = hidden.shape
    heads, hd = w["w_q"].shape[2:]
    rows, half, flat = batch // 2, width // 2, heads * hd
    ff = w["w_up"].shape[2]
    n_up = ff // UP_CHUNK
    vm = pl.BlockSpec(memory_space=pltpu.VMEM)
    any_ = pl.BlockSpec(memory_space=pl.ANY)
    dma = pltpu.SemaphoreType.DMA
    gain = pltpu.VMEM(w["norm_mlp"].shape, BF)
    ins = [("hidden", hidden)]
    outs = []
    scratch = [("ss_send", pltpu.VMEM((2, 8, 128), F32)), ("ss_recv", pltpu.VMEM((2, 3, 8, 128), F32)), ("ss_sem", dma((2, 2, 3))),
               ("h", pltpu.VMEM((batch, width), BF)), ("part", pltpu.VMEM((batch, half), F32)),
               ("v_hidden", pltpu.VMEM((batch, width), BF)), ("op_sem", dma((4,))), ("out_sem", dma((4,))),
               ("wup", pltpu.VMEM((width, ff if pre else 3 * flat), BF))]
    if pre:
        ins += [("ctx", ctx), ("g_mlp", w["norm_mlp"]), ("w_out", w["w_out"]), ("w_up", w["w_up"]), ("w_down", w["w_down"])]
        outs += [("x_out", (batch, width), BF, any_)]
        part = pltpu.VMEM((2, batch, half), BF)
        scratch += [("v_ctx", pltpu.VMEM((rows, heads, hd), F32)), ("v_g_mlp", gain),
                    ("wo", pltpu.VMEM((flat, width), BF)), ("wo_sem", dma((4,))), ("wup_sem", dma((n_up,))),
                    ("wdn", pltpu.VMEM((ff, width), BF)), ("wdn_sem", dma((n_up,))),
                    ("pair_send", part), ("pair_recv", part), ("pair_sem", dma((2, 2, PIECES))),
                    ("chip_send", part), ("chip_recv", part), ("chip_sem", dma((2, 2, PIECES))), ("share_sem", dma((2, 2, PIECES))),
                    ("ctx_all", pltpu.VMEM((batch, flat), BF)), ("ctx_sem", dma((2, 1))),
                    ("x_mid", pltpu.VMEM((batch, width), BF)), ("x_end", pltpu.VMEM((batch, width), BF)),
                    ("up_send", pltpu.VMEM((batch, ff), BF)), ("up_recv", pltpu.VMEM((batch, ff), BF)), ("up_sem", dma((2, n_up))),
                    ("act", pltpu.VMEM((batch, UP_CHUNK), BF)), ("acc", pltpu.VMEM((batch, width), F32))]
    if qkv:
        ins += [("g_attn", w["norm_attn"]), ("w_q", w["w_q"]), ("w_k", w["w_k"]), ("w_v", w["w_v"]), ("k_cache", w["k_cache"]), ("v_cache", w["v_cache"])]
        outs += [(n, (rows, heads, hd), F32, any_) for n in ("q", "k", "v")]
        outs += [(n, w["k_cache"].shape[1:], BF, vm) for n in ("k_now", "v_now")]
        share = pltpu.VMEM((3, rows, flat), BF)
        scratch += [("v_" + n, pltpu.VMEM((rows, heads, hd), F32)) for n in ("q", "k", "v")]
        scratch += [("v_g_attn", gain), ("cache_sem", dma((2, 4))),
                    ("wraw", pltpu.VMEM((width // RAW_CHUNK, RAW_CHUNK, heads, hd), BF)), ("wraw_sem", dma((width // RAW_CHUNK,))),
                    ("qkv_send", share), ("qkv_recv", share), ("qkv_own", share), ("qkv_sem", dma((2, 3)))]
    names = [n for n, *_ in ins] + [n for n, *_ in outs] + [n for n, _ in scratch]
    return pl.pallas_call(
        functools.partial(stage_body, pre, qkv, layer, names),
        out_shape=tuple(pltpu.VMEM(s, d) if n in ("k_now", "v_now") else jax.ShapeDtypeStruct(s, d) for n, s, d, _ in outs),
        in_specs=[any_ for _ in ins],
        out_specs=tuple(o[3] for o in outs),
        scratch_shapes=[s for _, s in scratch],
        compiler_params=pltpu.CompilerParams(collective_id=(1 if pre else 0) + (2 if qkv else 0), has_side_effects=True, vmem_limit_bytes=VMEM_LIMIT),
        name=f"stage_{int(pre)}{int(qkv)}",
    )(*[a for _, a in ins])


def solution(mesh):
    cache_spec = P(None, ("rep", "y"), None, "x", None)
    row_spec = P("rep", "y")
    proj_spec = P(None, "y", "x", None)
    head_spec = P(None, "x", None)
    in_specs = (row_spec, P("rep"), cache_spec, cache_spec, P(None, None, "x", None), P(None, "y"),
                proj_spec, proj_spec, proj_spec, head_spec, head_spec, P(None, "x", None, "y"),
                P(None, "y"), P(None, "y", "x"), P(None, "x", "y"))
    out_specs = (row_spec, cache_spec, cache_spec)

    def local_step(hidden, lengths, k_cache, v_cache, rel_table, norm_attn, w_q, w_k, w_v, bias_content, bias_pos, w_out, norm_mlp, w_up, w_down):
        layers, rows, seq, heads, hd = k_cache.shape
        merged = (layers, rows, seq * heads, hd)
        w = dict(norm_attn=norm_attn, w_q=w_q, w_k=w_k, w_v=w_v, norm_mlp=norm_mlp, w_up=w_up, w_down=w_down,
                 w_out=w_out.reshape(w_out.shape[0], -1, w_out.shape[3]), k_cache=k_cache.reshape(merged), v_cache=v_cache.reshape(merged))
        q, k, v, k_now, v_now = stage(False, True, 0, hidden, None, w)
        prev = None
        for layer in range(layers):
            ctx, *prev = attend_cache(layer, lengths, q, k, v, rel_table, bias_content, bias_pos, k_now, v_now, layers, prev)
            if layer + 1 < layers:
                hidden, q, k, v, k_now, v_now = stage(True, True, layer, hidden, ctx, w)
            else:
                hidden, = stage(True, False, layer, hidden, ctx, w)
        return hidden, prev[0].reshape(k_cache.shape), prev[1].reshape(v_cache.shape)

    return jax.shard_map(local_step, mesh=mesh, in_specs=in_specs, out_specs=out_specs, check_vma=False)
```

```python
import functools
import jax
import jax.numpy as jnp
from jax import lax
from jax.experimental import pallas as pl
from jax.experimental.pallas import tpu as pltpu
from jax.sharding import PartitionSpec as P

BF = jnp.bfloat16
F32 = jnp.float32

def attn_body(layer, group, len_ref, a_ref, c_ref, kn_ref, vn_ref, rext, k_in, v_in, *rest):
    ctx_ref, ko, vo, kbuf, vbuf, wsem = rest[-6:]
    rows, span, hd = kbuf.shape
    heads = a_ref.shape[1]
    seq = span // heads
    y = lax.axis_index("y")
    n_grp = rows // group

    @pl.loop(0, rows, unroll=4)
    def _(b):
        at = pl.ds(pl.multiple_of(len_ref[y * rows + b] * heads, heads), heads)
        kbuf[b, at] = kn_ref[b].astype(BF)
        vbuf[b, at] = vn_ref[b].astype(BF)

    col = lax.broadcasted_iota(jnp.int32, (heads, span), 1)
    row = lax.broadcasted_iota(jnp.int32, (heads, span), 0)
    own = (col % heads) == row
    pos = jnp.where(own, col // heads, 1 << 20)
    scale = hd ** -0.5

    def save(i):
        sl = pl.ds(i * group, group)
        return (pltpu.make_async_copy(kbuf.at[sl], ko.at[layer, sl], wsem.at[0, i]),
                pltpu.make_async_copy(vbuf.at[sl], vo.at[layer, sl], wsem.at[1, i]))

    @pl.loop(0, n_grp)
    def _(i):
        for c in save(i):
            c.start()

    @pl.loop(0, n_grp)
    def _(i):
        score = []
        for g in range(group):
            b = i * group + g
            ln = len_ref[y * rows + b]
            rr = rext[pl.ds(pl.multiple_of((seq - 1 - ln) * heads, heads), span)]
            lhs = jnp.concatenate([a_ref[b].astype(BF), c_ref[b].astype(BF)], axis=1)
            rhs = jnp.concatenate([kbuf[b], rr], axis=1)
            s = lax.dot_general(lhs, rhs, (((1,), (1,)), ((), ())), preferred_element_type=F32)
            score.append(jnp.where(pos <= ln, s * scale, -1e30))
        prob = []
        for g in range(group):
            s = score[g]
            m = jnp.max(s, axis=1, keepdims=True)
            e = jnp.exp(s - m)
            prob.append((e / jnp.sum(e, axis=1, keepdims=True)).astype(BF))
        for g in range(group):
            b = i * group + g
            o = jnp.dot(prob[g], vbuf[b], preferred_element_type=F32)
            ctx_ref[b] = o.astype(BF).astype(F32)

    @pl.loop(0, n_grp)
    def _(i):
        for c in save(i):
            c.wait()


def attend_cache(layer, lengths, fed, layers, prev, group=8):
    rows, span, hd = fed[-1].shape
    heads = fed[0].shape[1]
    any_ = pl.BlockSpec(memory_space=pltpu.HBM)
    vm = pl.BlockSpec(memory_space=pltpu.VMEM)
    n_grp = rows // group
    ins = [lengths] + [pltpu.with_memory_space_constraint(c, pltpu.VMEM) for c in fed]
    specs = [pl.BlockSpec(memory_space=pltpu.SMEM)] + [vm] * len(fed)
    alias = {6: 3, 7: 4}
    if prev is not None:
        ins += prev
        specs += [any_, any_]
        alias.update({8: 1, 9: 2})
    cache = jax.ShapeDtypeStruct((layers, rows, span, hd), BF)
    now = jax.ShapeDtypeStruct(fed[-1].shape, BF)
    return pl.pallas_call(
        functools.partial(attn_body, layer, group),
        out_shape=(pltpu.VMEM((rows, heads, hd), F32), cache, cache, now, now),
        in_specs=specs, out_specs=(vm, any_, any_, vm, vm), input_output_aliases=alias,
        scratch_shapes=[pltpu.SemaphoreType.DMA((2, n_grp))],
        compiler_params=pltpu.CompilerParams(vmem_limit_bytes=24 << 20),
        name=f"attend_{layer}")(*ins)[:3]


MESH = pl.DeviceIdType.MESH
EPS = 1e-6
UP_CHUNK = 512
PIECES = 4
VMEM_LIMIT = 45875200


def rows_to_cols(col):
    square = jnp.concatenate([col] * (128 // col.shape[0]), axis=0)
    return jnp.broadcast_to(jnp.sum(square.T, axis=0, keepdims=True), (8, 128))


def cols_to_rows(row, n):
    return jnp.broadcast_to(row[0:1], (128, 128)).T[:n, 0:1]


def stage_body(pre, qkv, layer, names, *refs):
    r = dict(zip(names, refs))
    batch, width = r["h"].shape
    ops = [n[2:] for n in names if n.startswith("v_") and n[2:] in names]
    operand = {n: pltpu.make_async_copy(r[n] if n != "rel" else r[n].at[layer + int(pre)], r["v_" + n], r["op_sem"].at[i]) for i, n in enumerate(ops)}
    for n in ops:
        operand[n].start()
    half = width // 2
    rows = batch // 2
    x = lax.axis_index("x")
    y = lax.axis_index("y")
    y_dev = {"y": 1 - y}
    core = x % 2
    pair_dev = {"x": x + 1 - 2 * core}
    far_dev = {"x": x + 1 - 2 * core, "y": 1 - y}
    chip_dev = {"x": (x + 2) % 4}
    qkv_layer = layer + 1 if pre else layer

    def remote(src, dst, sems, idx, dev):
        return pltpu.make_async_remote_copy(src, dst, r[sems].at[0, idx], r[sems].at[1, idx], device_id=dev, device_id_type=MESH)

    def wo_copy(i):
        n = r["wo"].shape[0] // 4
        return pltpu.make_async_copy(r["w_out"].at[layer, pl.ds(i * n, n)], r["wo"].at[pl.ds(i * n, n)], r["wo_sem"].at[i])

    def up_copy(i):
        cols = pl.ds(pl.multiple_of(i * UP_CHUNK, UP_CHUNK), UP_CHUNK)
        return pltpu.make_async_copy(r["w_up"].at[layer, :, cols], r["wup"].at[:, cols], r["wup_sem"].at[i])

    def down_copy(i):
        sl = pl.ds(i * UP_CHUNK, UP_CHUNK)
        return pltpu.make_async_copy(r["w_down"].at[layer, sl], r["wdn"].at[sl], r["wdn_sem"].at[i])

    slots, raw_rows = r["wraw"].shape[:2] if qkv else (1, width)
    turns = width // (slots * raw_rows)

    def cache_copies(i):
        src, dst = (("k_cache", "k_now"), ("v_cache", "v_now"))[i]
        n = r[dst].shape[0] // 4
        return [pltpu.make_async_copy(r[src].at[qkv_layer, pl.ds(j * n, n)], r[dst].at[pl.ds(j * n, n)], r["cache_sem"].at[i, j]) for j in range(4)]

    def raw_copy(m, turn, j):
        sl = pl.ds((turn * slots + j) * raw_rows, raw_rows)
        return pltpu.make_async_copy(r[("w_q", "w_k", "w_v")[m]].at[qkv_layer, sl], r["wraw"].at[j], r["wraw_sem"].at[j])

    def start_qkv():
        for j in range(slots):
            raw_copy(0, 0, j).start()

    def flatten(m):
        heads, hd = r["wraw"].shape[2:]
        for turn in range(turns):
            after = (m, turn + 1) if turn + 1 < turns else (m + 1, 0)

            @pl.loop(0, slots)
            def _(j):
                raw_copy(m, turn, j).wait()

                @pl.loop(0, raw_rows // 256)
                def _(b):
                    off = pl.multiple_of(b * 256, 256)
                    by_head = jnp.swapaxes(r["wraw"][j, pl.ds(off, 256)], 0, 1)
                    sl = pl.ds(pl.multiple_of((turn * slots + j) * raw_rows + off, 256), 256)
                    for hh in range(heads):
                        col = m * heads * hd + hh * hd
                        r["wup"][sl, col:col + hd] = by_head[hh]

                if after[0] < 3:
                    raw_copy(*after, j).start()

        first = 0 if not pre else 2
        if m == first:
            for c in cache_copies(0):
                c.start()
        if m == min(first + 1, 2):
            for c in cache_copies(1):
                c.start()

    def reverse_rel():
        operand["rel"].wait()
        seq, heads, hd = r["v_rel"].shape

        @pl.loop(0, seq, unroll=4)
        def _(t):
            r["rext"][pl.ds(pl.multiple_of((seq - 1 - t) * heads, heads), heads)] = r["v_rel"][t]
            r["rext"][pl.ds(pl.multiple_of((seq + t) * heads, heads), heads)] = jnp.zeros((heads, hd), BF)

    if pre:
        n_up = r["wup"].shape[1] // UP_CHUNK
        for i in range(4):
            wo_copy(i).start()

        @pl.loop(0, n_up)
        def _(i):
            up_copy(i).start()
    else:
        start_qkv()

    barrier = pltpu.get_barrier_semaphore()
    greet = [y_dev, pair_dev, chip_dev, far_dev] if pre else [y_dev]
    for dev in greet:
        pl.semaphore_signal(barrier, inc=1, device_id=dev, device_id_type=MESH)
    pl.semaphore_wait(barrier, len(greet))

    def row_sums(wide):
        sq = wide * wide
        part = sq[:, 0:128]
        for j in range(1, wide.shape[1] // 128):
            part = part + sq[:, j * 128:(j + 1) * 128]
        return part

    def sum_copy(slot, j, dev):
        return pltpu.make_async_remote_copy(r["ss_send"].at[slot], r["ss_recv"].at[slot, j], r["ss_sem"].at[0, slot, j], r["ss_sem"].at[1, slot, j],
                                            device_id=dev, device_id_type=MESH)

    def send_sums(slot, part, devs):
        r["ss_send"][slot] = rows_to_cols(part)
        for j, dev in enumerate(devs):
            sum_copy(slot, j, dev).start()

    def normalize(slot, devs, x_ref, gain_ref, gain_layer):
        for j, dev in enumerate(devs):
            sum_copy(slot, j, dev).wait()
        total = r["ss_send"][slot] + r["ss_recv"][slot, 0]
        if len(devs) > 1:
            total = total + (r["ss_recv"][slot, 1] + r["ss_recv"][slot, 2])
        inv = lax.rsqrt(cols_to_rows(total, batch) / (2 * width) + EPS)
        gain = gain_ref[pl.ds(gain_layer, 1)].astype(F32)
        r["h"][...] = (x_ref[...].astype(F32) * inv * gain).astype(BF)

    cells = [pair_dev, y_dev, far_dev]
    step = half // PIECES

    def piece(side, c):
        return pl.ds(pl.multiple_of(side * half + c * step, step), step)

    def reduce_x(slot, part_of, x_ref, out_ref, sums):
        def copy(kind, c):
            here = pl.ds(c * step, step)
            sems = r[kind + "_sem"]
            if kind == "share":
                src = dst = out_ref.at[:, piece(core, c)]
            else:
                src, dst = r[kind + "_send"].at[slot, :, here], r[kind + "_recv"].at[slot, :, here]
            return pltpu.make_async_remote_copy(src, dst, sems.at[0, slot, c], sems.at[1, slot, c],
                                                device_id=chip_dev if kind == "chip" else pair_dev, device_id_type=MESH)

        r["pair_send"][slot] = part_of(pl.ds(pl.multiple_of((1 - core) * half, half), half)).astype(BF)
        for c in range(PIECES):
            copy("pair", c).start()
        r["part"][...] = part_of(pl.ds(pl.multiple_of(core * half, half), half))
        for c in range(PIECES):
            copy("pair", c).wait()
            here = slice(c * step, (c + 1) * step)
            r["chip_send"][slot, :, here] = (r["part"][:, here] + r["pair_recv"][slot, :, here].astype(F32)).astype(BF)
            copy("chip", c).start()
        part = None
        for c in range(PIECES):
            copy("chip", c).wait()
            here = slice(c * step, (c + 1) * step)
            total = r["chip_send"][slot, :, here].astype(F32) + r["chip_recv"][slot, :, here].astype(F32)
            new = (x_ref[:, piece(core, c)].astype(F32) + total).astype(BF)
            out_ref[:, piece(core, c)] = new
            copy("share", c).start()
            if sums:
                add = row_sums(new.astype(F32))
                part = add if part is None else part + add
        if sums:
            send_sums(slot, part, cells)
        for c in range(PIECES):
            copy("share", c).wait()

    x_now = r["v_hidden"] if "hidden" in ops else r["hidden"]
    if pre:
        mine = pl.ds(pl.multiple_of(y * rows, rows), rows)
        heads, hd = r["ctx"].shape[1:]
        for hh in range(heads):
            r["ctx_all"][mine, hh * hd:(hh + 1) * hd] = r["ctx"][:, hh, :].astype(BF)
        cp = remote(r["ctx_all"].at[mine], r["ctx_all"].at[mine], "ctx_sem", 0, y_dev)
        cp.start()
        for i in range(4):
            wo_copy(i).wait()
        cp.wait()

        def wo_part(cols):
            return jnp.dot(r["ctx_all"][...], r["wo"][:, cols], preferred_element_type=F32)

        if "hidden" in ops:
            operand["hidden"].wait()
        operand["g_mlp"].wait()
        reduce_x(0, wo_part, x_now, r["x_mid"], True)

        @pl.loop(0, n_up)
        def _(i):
            down_copy(i).start()
        if qkv:
            start_qkv()

        normalize(0, cells, r["x_mid"], r["v_g_mlp"], layer)

        def exchange_up(i):
            cols = pl.ds(pl.multiple_of(i * UP_CHUNK, UP_CHUNK), UP_CHUNK)
            return remote(r["up_send"].at[:, cols], r["up_recv"].at[:, cols], "up_sem", i, y_dev)

        @pl.loop(0, n_up)
        def _(i):
            up_copy(i).wait()
            cols = pl.ds(pl.multiple_of(i * UP_CHUNK, UP_CHUNK), UP_CHUNK)
            r["up_send"][:, cols] = jnp.dot(r["h"][...], r["wup"][:, cols], preferred_element_type=F32).astype(BF)
            exchange_up(i).start()

        if qkv:
            for m in range(3):
                flatten(m)
            reverse_rel()

        def activate(i):
            cols = pl.ds(pl.multiple_of(i * UP_CHUNK, UP_CHUNK), UP_CHUNK)
            exchange_up(i).wait()
            m = (r["up_send"][:, cols].astype(F32) + r["up_recv"][:, cols].astype(F32)).astype(BF)
            r["act"][...] = jax.nn.gelu(m.astype(F32), approximate=True).astype(BF)

        r["acc"][...] = jnp.zeros_like(r["acc"])

        @pl.loop(0, n_up - 1)
        def _(i):
            down_copy(i).wait()
            activate(i)
            sl = pl.ds(pl.multiple_of(i * UP_CHUNK, UP_CHUNK), UP_CHUNK)
            r["acc"][...] += jnp.dot(r["act"][...], r["wdn"][sl, :], preferred_element_type=F32)

        down_copy(n_up - 1).wait()
        activate(n_up - 1)

        def down_part(cols):
            last = jnp.dot(r["act"][...], r["wdn"][pl.ds((n_up - 1) * UP_CHUNK, UP_CHUNK), cols], preferred_element_type=F32)
            return r["acc"][:, cols] + last

        reduce_x(1, down_part, r["x_mid"], r["x_end"], qkv)
        r["x_out"][...] = r["x_end"][...]
        x_now = r["x_end"]

    if qkv:
        heads, hd = r["wraw"].shape[2:]
        operand["g_attn"].wait()
        if pre:
            normalize(1, cells, x_now, r["v_g_attn"], qkv_layer)
        else:
            operand["hidden"].wait()
            send_sums(1, row_sums(x_now[...].astype(F32)), [y_dev])
            flatten(0)
            normalize(1, [y_dev], x_now, r["v_g_attn"], qkv_layer)
        mine = pl.ds(pl.multiple_of(y * rows, rows), rows)
        theirs = pl.ds(pl.multiple_of((1 - y) * rows, rows), rows)

        def swap(m):
            return remote(r["qkv_send"].at[m], r["qkv_recv"].at[m], "qkv_sem", m, y_dev)

        for m in range(3):
            if not pre and m > 0:
                flatten(m)
            for j in range(heads * hd // 256):
                cols = slice(j * 256, (j + 1) * 256)
                lanes = slice(m * heads * hd + j * 256, m * heads * hd + (j + 1) * 256)
                r["part"][:, cols] = jnp.dot(r["h"][...], r["wup"][:, lanes], preferred_element_type=F32)
            r["qkv_send"][m] = r["part"][theirs, :].astype(BF)
            swap(m).start()
            r["qkv_own"][m] = r["part"][mine, :].astype(BF)

        if not pre:
            reverse_rel()
        operand["bias_u"].wait()
        operand["bias_w"].wait()
        for m in range(3):
            swap(m).wait()
            full = (r["qkv_own"][m].astype(F32) + r["qkv_recv"][m].astype(F32)).astype(BF).astype(F32)
            for hh in range(heads):
                head = full[:, hh * hd:(hh + 1) * hd]
                if m:
                    r[("k", "v")[m - 1]][:, hh, :] = head
                else:
                    r["a"][:, hh, :] = (head + r["v_bias_u"][qkv_layer, hh:hh + 1].astype(F32)).astype(BF).astype(F32)
                    r["c"][:, hh, :] = (head + r["v_bias_w"][qkv_layer, hh:hh + 1].astype(F32)).astype(BF).astype(F32)
        for c in cache_copies(0) + cache_copies(1):
            c.wait()


def stage(pre, qkv, layer, hidden, ctx, w):
    batch, width = hidden.shape
    heads, hd = w["w_q"].shape[2:]
    rows, half, flat = batch // 2, width // 2, heads * hd
    ff = w["w_up"].shape[2]
    n_up = ff // UP_CHUNK
    vm = pl.BlockSpec(memory_space=pltpu.VMEM)
    any_ = pl.BlockSpec(memory_space=pltpu.HBM)
    dma = pltpu.SemaphoreType.DMA
    gain = pltpu.VMEM(w["norm_mlp"].shape, BF)
    ins = [("hidden", hidden)]
    placed = {"ctx"} if layer == 0 else {"ctx", "hidden"}
    outs = []
    scratch = [("ss_send", pltpu.VMEM((2, 8, 128), F32)), ("ss_recv", pltpu.VMEM((2, 3, 8, 128), F32)), ("ss_sem", dma((2, 2, 3))),
               ("h", pltpu.VMEM((batch, width), BF)), ("part", pltpu.VMEM((batch, half), F32)),
               ("op_sem", dma((6,))),
               ("wup", pltpu.VMEM((width, ff if pre else 3 * flat), BF))]
    if "hidden" not in placed:
        scratch += [("v_hidden", pltpu.VMEM((batch, width), BF))]
    if pre:
        ins += [("ctx", ctx), ("g_mlp", w["norm_mlp"]), ("w_out", w["w_out"]), ("w_up", w["w_up"]), ("w_down", w["w_down"])]
        outs += [("x_out", (batch, width), BF)]
        part = pltpu.VMEM((2, batch, half), BF)
        scratch += [("v_g_mlp", gain),
                    ("wo", pltpu.VMEM((flat, width), BF)), ("wo_sem", dma((4,))), ("wup_sem", dma((n_up,))),
                    ("wdn", pltpu.VMEM((ff, width), BF)), ("wdn_sem", dma((n_up,))),
                    ("pair_send", part), ("pair_recv", part), ("pair_sem", dma((2, 2, PIECES))),
                    ("chip_send", part), ("chip_recv", part), ("chip_sem", dma((2, 2, PIECES))), ("share_sem", dma((2, 2, PIECES))),
                    ("ctx_all", pltpu.VMEM((batch, flat), BF)), ("ctx_sem", dma((2, 1))),
                    ("x_mid", pltpu.VMEM((batch, width), BF)), ("x_end", pltpu.VMEM((batch, width), BF)),
                    ("up_send", pltpu.VMEM((batch, ff), BF)), ("up_recv", pltpu.VMEM((batch, ff), BF)), ("up_sem", dma((2, n_up))),
                    ("act", pltpu.VMEM((batch, UP_CHUNK), BF)), ("acc", pltpu.VMEM((batch, width), F32))]
    if qkv:
        ins += [("g_attn", w["norm_attn"]), ("w_q", w["w_q"]), ("w_k", w["w_k"]), ("w_v", w["w_v"]), ("k_cache", w["k_cache"]), ("v_cache", w["v_cache"])]
        ins += [("rel", w["rel"]), ("bias_u", w["bias_u"]), ("bias_w", w["bias_w"])]
        seq = w["rel"].shape[1]
        outs += [(n, (rows, heads, hd), F32) for n in ("a", "c", "k", "v")]
        outs += [("rext", (2 * seq * heads, hd), BF)]
        outs += [(n, w["k_cache"].shape[1:], BF) for n in ("k_now", "v_now")]
        share = pltpu.VMEM((3, rows, flat), BF)
        scratch += [("v_" + n, pltpu.VMEM(w[n].shape, BF)) for n in ("bias_u", "bias_w")]
        scratch += [("v_rel", pltpu.VMEM((seq, heads, hd), BF))]
        scratch += [("v_g_attn", gain), ("cache_sem", dma((2, 4))),
                    ("wraw", pltpu.VMEM((4, 256 if pre else 512, heads, hd), BF)), ("wraw_sem", dma((4,))),
                    ("qkv_send", share), ("qkv_recv", share), ("qkv_own", share), ("qkv_sem", dma((2, 3)))]
    names = [n for n, *_ in ins] + [n for n, *_ in outs] + [n for n, _ in scratch]
    args = [pltpu.with_memory_space_constraint(a, pltpu.VMEM if n in placed else pltpu.HBM) for n, a in ins]
    return pl.pallas_call(
        functools.partial(stage_body, pre, qkv, layer, names),
        out_shape=tuple(pltpu.VMEM(s, d) if qkv else jax.ShapeDtypeStruct(s, d) for _, s, d in outs),
        in_specs=[vm if n in placed else any_ for n, _ in ins],
        out_specs=tuple(vm for _ in outs),
        scratch_shapes=[s for _, s in scratch],
        compiler_params=pltpu.CompilerParams(collective_id=(1 if pre else 0) + (2 if qkv else 0), has_side_effects=True, vmem_limit_bytes=VMEM_LIMIT),
        name=f"stage_{int(pre)}{int(qkv)}",
    )(*args)


def solution(mesh):
    cache_spec = P(None, ("rep", "y"), None, "x", None)
    row_spec = P("rep", "y")
    proj_spec = P(None, "y", "x", None)
    head_spec = P(None, "x", None)
    in_specs = (row_spec, P("rep"), cache_spec, cache_spec, P(None, None, "x", None), P(None, "y"),
                proj_spec, proj_spec, proj_spec, head_spec, head_spec, P(None, "x", None, "y"),
                P(None, "y"), P(None, "y", "x"), P(None, "x", "y"))
    out_specs = (row_spec, cache_spec, cache_spec)

    def local_step(hidden, lengths, k_cache, v_cache, rel_table, norm_attn, w_q, w_k, w_v, bias_content, bias_pos, w_out, norm_mlp, w_up, w_down):
        layers, rows, seq, heads, hd = k_cache.shape
        merged = (layers, rows, seq * heads, hd)
        w = dict(norm_attn=norm_attn, w_q=w_q, w_k=w_k, w_v=w_v, norm_mlp=norm_mlp, w_up=w_up, w_down=w_down,
                 w_out=w_out.reshape(w_out.shape[0], -1, w_out.shape[3]), k_cache=k_cache.reshape(merged), v_cache=v_cache.reshape(merged),
                 rel=rel_table, bias_u=bias_content, bias_w=bias_pos)
        fed = stage(False, True, 0, hidden, None, w)
        prev = None
        for layer in range(layers):
            ctx, *prev = attend_cache(layer, lengths, fed, layers, prev)
            if layer + 1 < layers:
                hidden, *fed = stage(True, True, layer, hidden, ctx, w)
            else:
                hidden, = stage(True, False, layer, hidden, ctx, w)
        return hidden, prev[0].reshape(k_cache.shape), prev[1].reshape(v_cache.shape)

    return jax.shard_map(local_step, mesh=mesh, in_specs=in_specs, out_specs=out_specs, check_vma=False)
```

```python
import functools
import jax
import jax.numpy as jnp
from jax import lax
from jax.experimental import pallas as pl
from jax.experimental.pallas import tpu as pltpu
from jax.sharding import PartitionSpec as P

BF = jnp.bfloat16
F32 = jnp.float32

def attn_body(layer, group, len_ref, a_ref, c_ref, kn_ref, vn_ref, rext, k_in, v_in, *rest):
    ctx_ref, ko, vo, kbuf, vbuf, wsem = rest[-6:]
    rows, span, hd = kbuf.shape
    heads = a_ref.shape[1]
    seq = span // heads
    y = lax.axis_index("y")
    n_grp = rows // group

    @pl.loop(0, rows, unroll=4)
    def _(b):
        at = pl.ds(pl.multiple_of(len_ref[y * rows + b] * heads, heads), heads)
        kbuf[b, at] = kn_ref[b].astype(BF)
        vbuf[b, at] = vn_ref[b].astype(BF)

    col = lax.broadcasted_iota(jnp.int32, (heads, span), 1)
    row = lax.broadcasted_iota(jnp.int32, (heads, span), 0)
    own = (col % heads) == row
    pos = jnp.where(own, col // heads, 1 << 20)
    scale = hd ** -0.5

    def save(i):
        sl = pl.ds(i * group, group)
        return (pltpu.make_async_copy(kbuf.at[sl], ko.at[layer, sl], wsem.at[0, i]),
                pltpu.make_async_copy(vbuf.at[sl], vo.at[layer, sl], wsem.at[1, i]))

    @pl.loop(0, n_grp)
    def _(i):
        for c in save(i):
            c.start()

    @pl.loop(0, n_grp)
    def _(i):
        score = []
        for g in range(group):
            b = i * group + g
            ln = len_ref[y * rows + b]
            rr = rext[pl.ds(pl.multiple_of((seq - 1 - ln) * heads, heads), span)]
            lhs = jnp.concatenate([a_ref[b].astype(BF), c_ref[b].astype(BF)], axis=1)
            rhs = jnp.concatenate([kbuf[b], rr], axis=1)
            s = lax.dot_general(lhs, rhs, (((1,), (1,)), ((), ())), preferred_element_type=F32)
            score.append(jnp.where(pos <= ln, s * scale, -1e30))
        prob = []
        for g in range(group):
            s = score[g]
            m = jnp.max(s, axis=1, keepdims=True)
            e = jnp.exp(s - m)
            prob.append((e / jnp.sum(e, axis=1, keepdims=True)).astype(BF))
        for g in range(group):
            b = i * group + g
            o = jnp.dot(prob[g], vbuf[b], preferred_element_type=F32)
            ctx_ref[b] = o.astype(BF).astype(F32)

    @pl.loop(0, n_grp)
    def _(i):
        for c in save(i):
            c.wait()


def attend_cache(layer, lengths, fed, layers, prev, group=8):
    rows, span, hd = fed[-1].shape
    heads = fed[0].shape[1]
    any_ = pl.BlockSpec(memory_space=pltpu.HBM)
    vm = pl.BlockSpec(memory_space=pltpu.VMEM)
    n_grp = rows // group
    ins = [lengths] + [pltpu.with_memory_space_constraint(c, pltpu.VMEM) for c in fed]
    specs = [pl.BlockSpec(memory_space=pltpu.SMEM)] + [vm] * len(fed)
    alias = {6: 3, 7: 4}
    if prev is not None:
        ins += prev
        specs += [any_, any_]
        alias.update({8: 1, 9: 2})
    cache = jax.ShapeDtypeStruct((layers, rows, span, hd), BF)
    now = jax.ShapeDtypeStruct(fed[-1].shape, BF)
    return pl.pallas_call(
        functools.partial(attn_body, layer, group),
        out_shape=(pltpu.VMEM((rows, heads, hd), F32), cache, cache, now, now),
        in_specs=specs, out_specs=(vm, any_, any_, vm, vm), input_output_aliases=alias,
        scratch_shapes=[pltpu.SemaphoreType.DMA((2, n_grp))],
        compiler_params=pltpu.CompilerParams(vmem_limit_bytes=24 << 20),
        name=f"attend_{layer}")(*ins)[:3]


MESH = pl.DeviceIdType.MESH
EPS = 1e-6
UP_CHUNK = 512
VMEM_LIMIT = 45875200


def rows_to_cols(col):
    square = jnp.concatenate([col] * (128 // col.shape[0]), axis=0)
    return jnp.broadcast_to(jnp.sum(square.T, axis=0, keepdims=True), (8, 128))


def cols_to_rows(row, n):
    return jnp.broadcast_to(row[0:1], (128, 128)).T[:n, 0:1]


def stage_body(pre, qkv, layer, names, *refs):
    r = dict(zip(names, refs))
    batch, width = r["h"].shape
    ops = [n[2:] for n in names if n.startswith("v_") and n[2:] in names]
    operand = {n: pltpu.make_async_copy(r[n] if n != "rel" else r[n].at[layer + int(pre)], r["v_" + n], r["op_sem"].at[i]) for i, n in enumerate(ops)}
    for n in ops:
        operand[n].start()
    half = width // 2
    rows = batch // 2
    x = lax.axis_index("x")
    y = lax.axis_index("y")
    y_dev = {"y": 1 - y}
    core = x % 2
    pair_dev = {"x": x + 1 - 2 * core}
    mine = pl.ds(pl.multiple_of(y * rows, rows), rows)
    theirs = pl.ds(pl.multiple_of((1 - y) * rows, rows), rows)
    everyone = pl.ds(0, batch)
    chip_dev = {"x": (x + 2) % 4}
    qkv_layer = layer + 1 if pre else layer

    def remote(src, dst, sems, idx, dev):
        return pltpu.make_async_remote_copy(src, dst, r[sems].at[0, idx], r[sems].at[1, idx], device_id=dev, device_id_type=MESH)

    def wo_copy(i):
        n = r["wo"].shape[0] // 4
        return pltpu.make_async_copy(r["w_out"].at[layer, pl.ds(i * n, n)], r["wo"].at[pl.ds(i * n, n)], r["wo_sem"].at[i])

    def up_copy(i):
        cols = pl.ds(pl.multiple_of(i * UP_CHUNK, UP_CHUNK), UP_CHUNK)
        return pltpu.make_async_copy(r["w_up"].at[layer, :, cols], r["wup"].at[:, cols], r["wup_sem"].at[i])

    def down_copy(i):
        sl = pl.ds(i * UP_CHUNK, UP_CHUNK)
        return pltpu.make_async_copy(r["w_down"].at[layer, sl], r["wdn"].at[sl], r["wdn_sem"].at[i])

    slots, raw_rows = r["wraw"].shape[:2] if qkv else (1, width)
    turns = width // (slots * raw_rows)

    def cache_copies(i):
        src, dst = (("k_cache", "k_now"), ("v_cache", "v_now"))[i]
        n = r[dst].shape[0] // 4
        return [pltpu.make_async_copy(r[src].at[qkv_layer, pl.ds(j * n, n)], r[dst].at[pl.ds(j * n, n)], r["cache_sem"].at[i, j]) for j in range(4)]

    def raw_copy(m, turn, j):
        sl = pl.ds((turn * slots + j) * raw_rows, raw_rows)
        return pltpu.make_async_copy(r[("w_q", "w_k", "w_v")[m]].at[qkv_layer, sl], r["wraw"].at[j], r["wraw_sem"].at[j])

    def start_qkv():
        for j in range(slots):
            raw_copy(0, 0, j).start()

    def flatten(m):
        heads, hd = r["wraw"].shape[2:]
        for turn in range(turns):
            after = (m, turn + 1) if turn + 1 < turns else (m + 1, 0)

            @pl.loop(0, slots)
            def _(j):
                raw_copy(m, turn, j).wait()

                @pl.loop(0, raw_rows // 256)
                def _(b):
                    off = pl.multiple_of(b * 256, 256)
                    by_head = jnp.swapaxes(r["wraw"][j, pl.ds(off, 256)], 0, 1)
                    sl = pl.ds(pl.multiple_of((turn * slots + j) * raw_rows + off, 256), 256)
                    for hh in range(heads):
                        col = m * heads * hd + hh * hd
                        r["wup"][sl, col:col + hd] = by_head[hh]

                if after[0] < 3:
                    raw_copy(*after, j).start()

        if m < 2:
            for c in cache_copies(m):
                c.start()

    def reverse_rel():
        operand["rel"].wait()
        seq, heads, hd = r["v_rel"].shape

        @pl.loop(0, seq, unroll=4)
        def _(t):
            r["rext"][pl.ds(pl.multiple_of((seq - 1 - t) * heads, heads), heads)] = r["v_rel"][t]
            r["rext"][pl.ds(pl.multiple_of((seq + t) * heads, heads), heads)] = jnp.zeros((heads, hd), BF)

    if pre:
        n_up = r["wup"].shape[1] // UP_CHUNK
        for i in range(4):
            wo_copy(i).start()

        @pl.loop(0, n_up)
        def _(i):
            up_copy(i).start()
    else:
        start_qkv()

    barrier = pltpu.get_barrier_semaphore()
    greet = [y_dev, pair_dev, chip_dev] if pre else [y_dev]
    for dev in greet:
        pl.semaphore_signal(barrier, inc=1, device_id=dev, device_id_type=MESH)
    pl.semaphore_wait(barrier, len(greet))

    def row_sums(wide):
        sq = wide * wide
        part = sq[:, 0:128]
        for j in range(1, wide.shape[1] // 128):
            part = part + sq[:, j * 128:(j + 1) * 128]
        return part

    def sum_copy(slot):
        return remote(r["ss_send"].at[slot], r["ss_recv"].at[slot], "ss_sem", slot, y_dev)

    def inv_rms(sums, n):
        return lax.rsqrt(cols_to_rows(sums, n) / (2 * width) + EPS)

    def normalize(slot, x_ref, at, n, gain_ref, gain_layer):
        wide = x_ref[at].astype(F32)
        r["ss_send"][slot] = rows_to_cols(row_sums(wide))
        sum_copy(slot).start()
        gain = gain_ref[pl.ds(gain_layer, 1)].astype(F32)
        r["h"][at] = (x_ref[at].astype(F32) * inv_rms(r["ss_send"][slot], n) * gain).astype(BF)

    def factors(own_sums, peer_sums, n):
        whole = inv_rms(own_sums + peer_sums, n)
        return whole / inv_rms(own_sums, n), whole / inv_rms(peer_sums, n)

    def half_of(side):
        return pl.ds(pl.multiple_of(side * half, half), half)

    def reducer(slot, bank, at, pieces, part_of, x_ref, out_ref):
        step = half // pieces

        def copy(kind, c=0):
            here = pl.ds(c * step, step) if kind == "chip" else pl.ds(0, half)
            if kind == "share":
                src = dst = out_ref.at[at, pl.ds(pl.multiple_of(core * half + c * step, step), step)]
            else:
                src, dst = r[kind + "_send"].at[bank, at, here], r[kind + "_recv"].at[bank, at, here]
            sems = r[kind + "_sem"]
            return pltpu.make_async_remote_copy(src, dst, sems.at[0, slot, c], sems.at[1, slot, c],
                                                device_id=chip_dev if kind == "chip" else pair_dev, device_id_type=MESH)

        def begin():
            r["pair_send"][bank, at] = part_of(half_of(1 - core)).astype(BF)
            copy("pair").start()
            r["part"][at] = part_of(half_of(core))

        def cross():
            copy("pair").wait()
            for c in range(pieces):
                here = slice(c * step, (c + 1) * step)
                r["chip_send"][bank, at, here] = (r["part"][at, here] + r["pair_recv"][bank, at, here].astype(F32)).astype(BF)
                copy("chip", c).start()

        def land():
            for c in range(pieces):
                copy("chip", c).wait()
                here = slice(c * step, (c + 1) * step)
                cols = pl.ds(pl.multiple_of(core * half + c * step, step), step)
                total = r["chip_send"][bank, at, here].astype(F32) + r["chip_recv"][bank, at, here].astype(F32)
                out_ref[at, cols] = (x_ref[at, cols].astype(F32) + total).astype(BF)
                copy("share", c).start()

        def finish():
            for c in range(pieces):
                copy("share", c).wait()

        return begin, cross, land, finish

    x_now = r["v_hidden"] if "hidden" in ops else r["hidden"]
    if pre:
        heads, hd = r["ctx"].shape[1:]
        for hh in range(heads):
            r["ctx_all"][mine, hh * hd:(hh + 1) * hd] = r["ctx"][:, hh, :].astype(BF)
        ctx_copy = remote(r["ctx_all"].at[mine], r["ctx_all"].at[mine], "ctx_sem", 0, y_dev)
        ctx_copy.start()

        def wo_part(at):
            return lambda cols: jnp.dot(r["ctx_all"][at], r["wo"][:, cols], preferred_element_type=F32)

        near = reducer(0, 0, mine, 2, wo_part(mine), x_now, r["x_mid"])
        far = reducer(1, 0, theirs, 2, wo_part(theirs), x_now, r["x_mid"])
        for i in range(4):
            wo_copy(i).wait()
        near[0]()
        near[1]()

        @pl.loop(0, n_up)
        def _(i):
            down_copy(i).start()
        if qkv:
            start_qkv()
        ctx_copy.wait()
        far[0]()
        far[1]()
        if "hidden" in ops:
            operand["hidden"].wait()
        operand["g_mlp"].wait()

        def exchange_up(g, at, i):
            cols = pl.ds(pl.multiple_of(i * UP_CHUNK, UP_CHUNK), UP_CHUNK)
            return pltpu.make_async_remote_copy(r["up_send"].at[at, cols], r["up_recv"].at[at, cols], r["up_sem"].at[0, g, i], r["up_sem"].at[1, g, i],
                                                device_id=y_dev, device_id_type=MESH)

        def send_up(g, at):
            normalize(g, r["x_mid"], at, rows, r["v_g_mlp"], layer)

            @pl.loop(0, n_up)
            def _(i):
                if g == 0:
                    up_copy(i).wait()
                cols = pl.ds(pl.multiple_of(i * UP_CHUNK, UP_CHUNK), UP_CHUNK)
                r["up_send"][at, cols] = jnp.dot(r["h"][at], r["wup"][:, cols], preferred_element_type=F32).astype(BF)
                exchange_up(g, at, i).start()

        near[2]()
        near[3]()
        send_up(0, mine)
        far[2]()
        far[3]()
        send_up(1, theirs)

        if qkv:
            flatten(0)

        for g in range(2):
            sum_copy(g).wait()
        for g, at in enumerate((mine, theirs)):
            for j, f in enumerate(factors(r["ss_send"][g], r["ss_recv"][1 - g], rows)):
                r["fac"][j, at] = jnp.broadcast_to(f, (rows, 128))

        def activate(i):
            cols = pl.ds(pl.multiple_of(i * UP_CHUNK, UP_CHUNK), UP_CHUNK)
            exchange_up(0, mine, i).wait()
            exchange_up(1, theirs, i).wait()
            m = r["up_send"][:, cols].astype(F32) * r["fac"][0][:, 0:1] + r["up_recv"][:, cols].astype(F32) * r["fac"][1][:, 0:1]
            r["act"][...] = jax.nn.gelu(m.astype(BF).astype(F32), approximate=True).astype(BF)

        r["acc"][...] = jnp.zeros_like(r["acc"])

        @pl.loop(0, n_up - 1)
        def _(i):
            down_copy(i).wait()
            activate(i)
            sl = pl.ds(pl.multiple_of(i * UP_CHUNK, UP_CHUNK), UP_CHUNK)
            r["acc"][...] += jnp.dot(r["act"][...], r["wdn"][sl, :], preferred_element_type=F32)

        down_copy(n_up - 1).wait()
        activate(n_up - 1)

        def down_part(cols):
            last = jnp.dot(r["act"][...], r["wdn"][pl.ds((n_up - 1) * UP_CHUNK, UP_CHUNK), cols], preferred_element_type=F32)
            return r["acc"][:, cols] + last

        begin, cross, land, finish = reducer(2, 1, everyone, 4, down_part, r["x_mid"], r["x_end"])
        begin()
        cross()
        if qkv:
            flatten(1)
            flatten(2)
            reverse_rel()
        land()
        finish()
        r["x_out"][...] = r["x_end"][...]
        x_now = r["x_end"]

    if qkv:
        heads, hd = r["wraw"].shape[2:]
        operand["g_attn"].wait()
        if not pre:
            operand["hidden"].wait()
        normalize(2, x_now, everyone, batch, r["v_g_attn"], qkv_layer)

        def swap(m):
            return remote(r["qkv_send"].at[m], r["qkv_recv"].at[m], "qkv_sem", m, y_dev)

        for m in range(3):
            if not pre:
                flatten(m)
            for j in range(heads * hd // 256):
                cols = slice(j * 256, (j + 1) * 256)
                lanes = slice(m * heads * hd + j * 256, m * heads * hd + (j + 1) * 256)
                r["part"][:, cols] = jnp.dot(r["h"][...], r["wup"][:, lanes], preferred_element_type=F32)
            r["qkv_send"][m] = r["part"][theirs, :].astype(BF)
            swap(m).start()
            r["qkv_own"][m] = r["part"][mine, :].astype(BF)

        if not pre:
            reverse_rel()
        operand["bias_u"].wait()
        operand["bias_w"].wait()
        sum_copy(2).wait()
        for j, f in enumerate(factors(r["ss_send"][2], r["ss_recv"][2], batch)):
            r["fac"][j] = jnp.broadcast_to(f, (batch, 128))
        own_fac, peer_fac = (r["fac"][j, mine][:, 0:1] for j in range(2))
        for m in range(3):
            swap(m).wait()
            full = (r["qkv_own"][m].astype(F32) * own_fac + r["qkv_recv"][m].astype(F32) * peer_fac).astype(BF).astype(F32)
            for hh in range(heads):
                head = full[:, hh * hd:(hh + 1) * hd]
                if m:
                    r[("k", "v")[m - 1]][:, hh, :] = head
                else:
                    r["a"][:, hh, :] = (head + r["v_bias_u"][qkv_layer, hh:hh + 1].astype(F32)).astype(BF).astype(F32)
                    r["c"][:, hh, :] = (head + r["v_bias_w"][qkv_layer, hh:hh + 1].astype(F32)).astype(BF).astype(F32)
        for c in cache_copies(0) + cache_copies(1):
            c.wait()


def stage(pre, qkv, layer, hidden, ctx, w):
    batch, width = hidden.shape
    heads, hd = w["w_q"].shape[2:]
    rows, half, flat = batch // 2, width // 2, heads * hd
    ff = w["w_up"].shape[2]
    n_up = ff // UP_CHUNK
    vm = pl.BlockSpec(memory_space=pltpu.VMEM)
    any_ = pl.BlockSpec(memory_space=pltpu.HBM)
    dma = pltpu.SemaphoreType.DMA
    gain = pltpu.VMEM(w["norm_mlp"].shape, BF)
    ins = [("hidden", hidden)]
    placed = {"ctx"} if layer == 0 else {"ctx", "hidden"}
    outs = []
    scratch = [("ss_send", pltpu.VMEM((3, 8, 128), F32)), ("ss_recv", pltpu.VMEM((3, 8, 128), F32)), ("ss_sem", dma((2, 3))),
               ("fac", pltpu.VMEM((2, batch, 128), F32)),
               ("h", pltpu.VMEM((batch, width), BF)), ("part", pltpu.VMEM((batch, half), F32)),
               ("op_sem", dma((6,))),
               ("wup", pltpu.VMEM((width, ff if pre else 3 * flat), BF))]
    if "hidden" not in placed:
        scratch += [("v_hidden", pltpu.VMEM((batch, width), BF))]
    if pre:
        ins += [("ctx", ctx), ("g_mlp", w["norm_mlp"]), ("w_out", w["w_out"]), ("w_up", w["w_up"]), ("w_down", w["w_down"])]
        outs += [("x_out", (batch, width), BF)]
        part = pltpu.VMEM((2, batch, half), BF)
        scratch += [("v_g_mlp", gain),
                    ("wo", pltpu.VMEM((flat, width), BF)), ("wo_sem", dma((4,))), ("wup_sem", dma((n_up,))),
                    ("wdn", pltpu.VMEM((ff, width), BF)), ("wdn_sem", dma((n_up,))),
                    ("pair_send", part), ("pair_recv", part), ("pair_sem", dma((2, 3, 4))),
                    ("chip_send", part), ("chip_recv", part), ("chip_sem", dma((2, 3, 4))), ("share_sem", dma((2, 3, 4))),
                    ("ctx_all", pltpu.VMEM((batch, flat), BF)), ("ctx_sem", dma((2, 1))),
                    ("x_mid", pltpu.VMEM((batch, width), BF)), ("x_end", pltpu.VMEM((batch, width), BF)),
                    ("up_send", pltpu.VMEM((batch, ff), BF)), ("up_recv", pltpu.VMEM((batch, ff), BF)), ("up_sem", dma((2, 2, n_up))),
                    ("act", pltpu.VMEM((batch, UP_CHUNK), BF)), ("acc", pltpu.VMEM((batch, width), F32))]
    if qkv:
        ins += [("g_attn", w["norm_attn"]), ("w_q", w["w_q"]), ("w_k", w["w_k"]), ("w_v", w["w_v"]), ("k_cache", w["k_cache"]), ("v_cache", w["v_cache"])]
        ins += [("rel", w["rel"]), ("bias_u", w["bias_u"]), ("bias_w", w["bias_w"])]
        seq = w["rel"].shape[1]
        outs += [(n, (rows, heads, hd), F32) for n in ("a", "c", "k", "v")]
        outs += [("rext", (2 * seq * heads, hd), BF)]
        outs += [(n, w["k_cache"].shape[1:], BF) for n in ("k_now", "v_now")]
        share = pltpu.VMEM((3, rows, flat), BF)
        scratch += [("v_" + n, pltpu.VMEM(w[n].shape, BF)) for n in ("bias_u", "bias_w")]
        scratch += [("v_rel", pltpu.VMEM((seq, heads, hd), BF))]
        scratch += [("v_g_attn", gain), ("cache_sem", dma((2, 4))),
                    ("wraw", pltpu.VMEM((4, 256 if pre else 512, heads, hd), BF)), ("wraw_sem", dma((4,))),
                    ("qkv_send", share), ("qkv_recv", share), ("qkv_own", share), ("qkv_sem", dma((2, 3)))]
    names = [n for n, *_ in ins] + [n for n, *_ in outs] + [n for n, _ in scratch]
    args = [pltpu.with_memory_space_constraint(a, pltpu.VMEM if n in placed else pltpu.HBM) for n, a in ins]
    return pl.pallas_call(
        functools.partial(stage_body, pre, qkv, layer, names),
        out_shape=tuple(pltpu.VMEM(s, d) if qkv else jax.ShapeDtypeStruct(s, d) for _, s, d in outs),
        in_specs=[vm if n in placed else any_ for n, _ in ins],
        out_specs=tuple(vm for _ in outs),
        scratch_shapes=[s for _, s in scratch],
        compiler_params=pltpu.CompilerParams(collective_id=(1 if pre else 0) + (2 if qkv else 0), has_side_effects=True, vmem_limit_bytes=VMEM_LIMIT),
        name=f"stage_{int(pre)}{int(qkv)}",
    )(*args)


def solution(mesh):
    cache_spec = P(None, ("rep", "y"), None, "x", None)
    row_spec = P("rep", "y")
    proj_spec = P(None, "y", "x", None)
    head_spec = P(None, "x", None)
    in_specs = (row_spec, P("rep"), cache_spec, cache_spec, P(None, None, "x", None), P(None, "y"),
                proj_spec, proj_spec, proj_spec, head_spec, head_spec, P(None, "x", None, "y"),
                P(None, "y"), P(None, "y", "x"), P(None, "x", "y"))
    out_specs = (row_spec, cache_spec, cache_spec)

    def local_step(hidden, lengths, k_cache, v_cache, rel_table, norm_attn, w_q, w_k, w_v, bias_content, bias_pos, w_out, norm_mlp, w_up, w_down):
        layers, rows, seq, heads, hd = k_cache.shape
        merged = (layers, rows, seq * heads, hd)
        w = dict(norm_attn=norm_attn, w_q=w_q, w_k=w_k, w_v=w_v, norm_mlp=norm_mlp, w_up=w_up, w_down=w_down,
                 w_out=w_out.reshape(w_out.shape[0], -1, w_out.shape[3]), k_cache=k_cache.reshape(merged), v_cache=v_cache.reshape(merged),
                 rel=rel_table, bias_u=bias_content, bias_w=bias_pos)
        fed = stage(False, True, 0, hidden, None, w)
        prev = None
        for layer in range(layers):
            ctx, *prev = attend_cache(layer, lengths, fed, layers, prev)
            if layer + 1 < layers:
                hidden, *fed = stage(True, True, layer, hidden, ctx, w)
            else:
                hidden, = stage(True, False, layer, hidden, ctx, w)
        return hidden, prev[0].reshape(k_cache.shape), prev[1].reshape(v_cache.shape)

    return jax.shard_map(local_step, mesh=mesh, in_specs=in_specs, out_specs=out_specs, check_vma=False)
```

```python
import functools
import jax
import jax.numpy as jnp
from jax import lax
from jax.experimental import pallas as pl
from jax.experimental.pallas import tpu as pltpu
from jax.sharding import PartitionSpec as P

BF = jnp.bfloat16
F32 = jnp.float32

def attn_body(layer, group, len_ref, a_ref, c_ref, kn_ref, vn_ref, rext, k_in, v_in, *rest):
    ctx_ref, ko, vo, kbuf, vbuf, wsem = rest[-6:]
    rows, span, hd = kbuf.shape
    heads = a_ref.shape[1]
    seq = span // heads
    y = lax.axis_index("y")
    n_grp = rows // group

    @pl.loop(0, rows, unroll=4)
    def _(b):
        at = pl.ds(pl.multiple_of(len_ref[y * rows + b] * heads, heads), heads)
        kbuf[b, at] = kn_ref[b].astype(BF)
        vbuf[b, at] = vn_ref[b].astype(BF)

    col = lax.broadcasted_iota(jnp.int32, (heads, span), 1)
    row = lax.broadcasted_iota(jnp.int32, (heads, span), 0)
    own = (col % heads) == row
    pos = jnp.where(own, col // heads, 1 << 20)
    scale = hd ** -0.5

    def save(i):
        sl = pl.ds(i * group, group)
        return (pltpu.make_async_copy(kbuf.at[sl], ko.at[layer, sl], wsem.at[0, i]),
                pltpu.make_async_copy(vbuf.at[sl], vo.at[layer, sl], wsem.at[1, i]))

    @pl.loop(0, n_grp)
    def _(i):
        for c in save(i):
            c.start()

    @pl.loop(0, n_grp)
    def _(i):
        score = []
        for g in range(group):
            b = i * group + g
            ln = len_ref[y * rows + b]
            rr = rext[pl.ds(pl.multiple_of((seq - 1 - ln) * heads, heads), span)]
            lhs = jnp.concatenate([a_ref[b].astype(BF), c_ref[b].astype(BF)], axis=1)
            rhs = jnp.concatenate([kbuf[b], rr], axis=1)
            s = lax.dot_general(lhs, rhs, (((1,), (1,)), ((), ())), preferred_element_type=F32)
            score.append(jnp.where(pos <= ln, s * scale, -1e30))
        prob = []
        for g in range(group):
            s = score[g]
            m = jnp.max(s, axis=1, keepdims=True)
            e = jnp.exp(s - m)
            prob.append((e / jnp.sum(e, axis=1, keepdims=True)).astype(BF))
        for g in range(group):
            b = i * group + g
            o = jnp.dot(prob[g], vbuf[b], preferred_element_type=F32)
            ctx_ref[b] = o.astype(BF).astype(F32)

    @pl.loop(0, n_grp)
    def _(i):
        for c in save(i):
            c.wait()


def attend_cache(layer, lengths, fed, layers, prev, group=8):
    rows, span, hd = fed[-1].shape
    heads = fed[0].shape[1]
    any_ = pl.BlockSpec(memory_space=pltpu.HBM)
    vm = pl.BlockSpec(memory_space=pltpu.VMEM)
    n_grp = rows // group
    ins = [lengths] + [pltpu.with_memory_space_constraint(c, pltpu.VMEM) for c in fed]
    specs = [pl.BlockSpec(memory_space=pltpu.SMEM)] + [vm] * len(fed)
    alias = {6: 3, 7: 4}
    if prev is not None:
        ins += prev
        specs += [any_, any_]
        alias.update({8: 1, 9: 2})
    cache = jax.ShapeDtypeStruct((layers, rows, span, hd), BF)
    now = jax.ShapeDtypeStruct(fed[-1].shape, BF)
    return pl.pallas_call(
        functools.partial(attn_body, layer, group),
        out_shape=(pltpu.VMEM((rows, heads, hd), F32), cache, cache, now, now),
        in_specs=specs, out_specs=(vm, any_, any_, vm, vm), input_output_aliases=alias,
        scratch_shapes=[pltpu.SemaphoreType.DMA((2, n_grp))],
        compiler_params=pltpu.CompilerParams(vmem_limit_bytes=24 << 20),
        name=f"attend_{layer}")(*ins)[:3]


MESH = pl.DeviceIdType.MESH
EPS = 1e-6
UP_CHUNK = 512
VMEM_LIMIT = 46399488


def rows_to_cols(col):
    square = jnp.concatenate([col] * (128 // col.shape[0]), axis=0)
    return jnp.broadcast_to(jnp.sum(square.T, axis=0, keepdims=True), (8, 128))


def cols_to_rows(row, n):
    return jnp.broadcast_to(row[0:1], (128, 128)).T[:n, 0:1]


def stage_body(pre, qkv, layer, names, *refs):
    r = dict(zip(names, refs))
    batch, width = r["h"].shape
    ops = [n[2:] for n in names if n.startswith("v_") and n[2:] in names]
    operand = {n: pltpu.make_async_copy(r[n] if n != "rel" else r[n].at[layer + int(pre)], r["v_" + n], r["op_sem"].at[i]) for i, n in enumerate(ops)}
    for n in ops:
        operand[n].start()
    half = width // 2
    rows = batch // 2
    x = lax.axis_index("x")
    y = lax.axis_index("y")
    y_dev = {"y": 1 - y}
    core = x % 2
    pair_dev = {"x": x + 1 - 2 * core}
    mine = pl.ds(pl.multiple_of(y * rows, rows), rows)
    theirs = pl.ds(pl.multiple_of((1 - y) * rows, rows), rows)
    everyone = pl.ds(0, batch)
    chip_dev = {"x": (x + 2) % 4}
    qkv_layer = layer + 1 if pre else layer

    def remote(src, dst, sems, idx, dev):
        return pltpu.make_async_remote_copy(src, dst, r[sems].at[0, idx], r[sems].at[1, idx], device_id=dev, device_id_type=MESH)

    def wo_copy(i):
        n = r["wo"].shape[0] // 4
        return pltpu.make_async_copy(r["w_out"].at[layer, pl.ds(i * n, n)], r["wo"].at[pl.ds(i * n, n)], r["wo_sem"].at[i])

    def up_copy(i):
        cols = pl.ds(pl.multiple_of(i * UP_CHUNK, UP_CHUNK), UP_CHUNK)
        return pltpu.make_async_copy(r["w_up"].at[layer, :, cols], r["wup"].at[:, cols], r["wup_sem"].at[i])

    def down_copy(i):
        sl = pl.ds(i * UP_CHUNK, UP_CHUNK)
        return pltpu.make_async_copy(r["w_down"].at[layer, sl], r["wdn"].at[sl], r["wdn_sem"].at[i])

    slots, raw_rows = r["wraw"].shape[:2] if qkv else (1, width)
    turns = width // (slots * raw_rows)

    def cache_copies(i):
        src, dst = (("k_cache", "k_now"), ("v_cache", "v_now"))[i]
        n = r[dst].shape[0] // 4
        return [pltpu.make_async_copy(r[src].at[qkv_layer, pl.ds(j * n, n)], r[dst].at[pl.ds(j * n, n)], r["cache_sem"].at[i, j]) for j in range(4)]

    def raw_copy(m, turn, j):
        sl = pl.ds((turn * slots + j) * raw_rows, raw_rows)
        return pltpu.make_async_copy(r[("w_q", "w_k", "w_v")[m]].at[qkv_layer, sl], r["wraw"].at[j], r["wraw_sem"].at[j])

    def start_qkv():
        for j in range(slots):
            raw_copy(0, 0, j).start()

    def flatten(m):
        heads, hd = r["wraw"].shape[2:]
        for turn in range(turns):
            after = (m, turn + 1) if turn + 1 < turns else (m + 1, 0)

            @pl.loop(0, slots)
            def _(j):
                raw_copy(m, turn, j).wait()

                @pl.loop(0, raw_rows // 256)
                def _(b):
                    off = pl.multiple_of(b * 256, 256)
                    by_head = jnp.swapaxes(r["wraw"][j, pl.ds(off, 256)], 0, 1)
                    sl = pl.ds(pl.multiple_of((turn * slots + j) * raw_rows + off, 256), 256)
                    for hh in range(heads):
                        col = m * heads * hd + hh * hd
                        r["wup"][sl, col:col + hd] = by_head[hh]

                if after[0] < 3:
                    raw_copy(*after, j).start()

        if m < 2 and not pre:
            for c in cache_copies(m):
                c.start()

    def project(m, at, dst):
        lanes = dst.shape[1]
        for j in range(lanes // 256):
            cols = slice(j * 256, (j + 1) * 256)
            dst[:, cols] = jnp.dot(r["h"][at], r["wup"][:, m * lanes + j * 256:m * lanes + (j + 1) * 256], preferred_element_type=F32).astype(dst.dtype)

    def swap(m):
        return remote(r["qkv_send"].at[m], r["qkv_recv"].at[m], "qkv_sem", m, y_dev)

    def send_rows(m):
        project(m, theirs, r["qkv_send"].at[m])
        swap(m).start()

    def reverse_rel():
        operand["rel"].wait()
        seq, heads, hd = r["v_rel"].shape

        @pl.loop(0, seq, unroll=4)
        def _(t):
            r["rext"][pl.ds(pl.multiple_of((seq - 1 - t) * heads, heads), heads)] = r["v_rel"][t]
            r["rext"][pl.ds(pl.multiple_of((seq + t) * heads, heads), heads)] = jnp.zeros((heads, hd), BF)

    if pre:
        n_up = r["wup"].shape[1] // UP_CHUNK
        for i in range(4):
            wo_copy(i).start()

        @pl.loop(0, n_up)
        def _(i):
            up_copy(i).start()
    else:
        start_qkv()

    barrier = pltpu.get_barrier_semaphore()
    greet = [y_dev, pair_dev, chip_dev] if pre else [y_dev]
    for dev in greet:
        pl.semaphore_signal(barrier, inc=1, device_id=dev, device_id_type=MESH)
    pl.semaphore_wait(barrier, len(greet))

    def row_sums(wide):
        sq = wide * wide
        part = sq[:, 0:128]
        for j in range(1, wide.shape[1] // 128):
            part = part + sq[:, j * 128:(j + 1) * 128]
        return part

    def sum_copy(slot):
        return remote(r["ss_send"].at[slot], r["ss_recv"].at[slot], "ss_sem", slot, y_dev)

    def inv_rms(sums):
        return lax.rsqrt(cols_to_rows(sums, rows) / (2 * width) + EPS)

    def normalize(slot, x_ref, at, gain_ref, gain_layer, send=True):
        wide = x_ref[at].astype(F32)
        r["ss_send"][slot] = rows_to_cols(row_sums(wide))
        if send:
            sum_copy(slot).start()
        gain = gain_ref[pl.ds(gain_layer, 1)].astype(F32)
        r["h"][at] = (x_ref[at].astype(F32) * inv_rms(r["ss_send"][slot]) * gain).astype(BF)

    def factors(own_sums, peer_sums):
        whole = inv_rms(own_sums + peer_sums)
        return whole / jnp.maximum(inv_rms(own_sums), 1e-30), whole / jnp.maximum(inv_rms(peer_sums), 1e-30)

    def half_of(side):
        return pl.ds(pl.multiple_of(side * half, half), half)

    def reducer(slot, bank, at, pieces, part_of, x_ref, out_ref):
        step = half // pieces

        def copy(kind, c=0):
            here = pl.ds(c * step, step) if kind == "chip" else pl.ds(0, half)
            if kind == "share":
                src = dst = out_ref.at[at, pl.ds(pl.multiple_of(core * half + c * step, step), step)]
            else:
                src, dst = r[kind + "_send"].at[at, here], r[kind + "_recv"].at[bank, at, here]
            sems = r[kind + "_sem"]
            return pltpu.make_async_remote_copy(src, dst, sems.at[0, slot, c], sems.at[1, slot, c],
                                                device_id=chip_dev if kind == "chip" else pair_dev, device_id_type=MESH)

        def begin():
            r["pair_send"][at] = part_of(half_of(1 - core)).astype(BF)
            copy("pair").start()
            r["part"][at] = part_of(half_of(core))

        def cross():
            copy("pair").wait()
            for c in range(pieces):
                here = slice(c * step, (c + 1) * step)
                r["chip_send"][at, here] = (r["part"][at, here] + r["pair_recv"][bank, at, here].astype(F32)).astype(BF)
                copy("chip", c).start()

        def land():
            for c in range(pieces):
                copy("chip", c).wait()
                here = slice(c * step, (c + 1) * step)
                cols = pl.ds(pl.multiple_of(core * half + c * step, step), step)
                total = r["chip_send"][at, here].astype(F32) + r["chip_recv"][bank, at, here].astype(F32)
                out_ref[at, cols] = (x_ref[at, cols].astype(F32) + total).astype(BF)
                copy("share", c).start()

        def finish():
            for c in range(pieces):
                copy("share", c).wait()

        return begin, cross, land, finish

    x_now = r["v_hidden"] if "hidden" in ops else r["hidden"]
    if pre:
        heads, hd = r["ctx"].shape[1:]
        for hh in range(heads):
            r["ctx_all"][mine, hh * hd:(hh + 1) * hd] = r["ctx"][:, hh, :].astype(BF)
        ctx_copy = remote(r["ctx_all"].at[mine], r["ctx_all"].at[mine], "ctx_sem", 0, y_dev)
        ctx_copy.start()

        def wo_part(at):
            return lambda cols: jnp.dot(r["ctx_all"][at], r["wo"][:, cols], preferred_element_type=F32)

        near = reducer(0, 0, mine, 2, wo_part(mine), x_now, r["x_mid"])
        far = reducer(1, 0, theirs, 2, wo_part(theirs), x_now, r["x_mid"])
        for i in range(4):
            wo_copy(i).wait()
        near[0]()
        near[1]()

        @pl.loop(0, n_up)
        def _(i):
            down_copy(i).start()
        if qkv:
            start_qkv()
        ctx_copy.wait()
        far[0]()
        far[1]()
        if "hidden" in ops:
            operand["hidden"].wait()
        operand["g_mlp"].wait()

        ff = r["wup"].shape[1]

        def exchange_up(g, at, i):
            cols = pl.ds(i * UP_CHUNK, UP_CHUNK)
            return pltpu.make_async_remote_copy(r["up_send"].at[at, cols], r["up_recv"].at[at, cols], r["up_sem"].at[0, g, i], r["up_sem"].at[1, g, i],
                                                device_id=y_dev, device_id_type=MESH)

        def send_up(g, at, first, end):
            cols = slice(first * UP_CHUNK, end * UP_CHUNK)
            if g == 0:
                for i in range(first, end):
                    up_copy(i).wait()
            r["up_send"][at, cols] = jnp.dot(r["h"][at], r["wup"][:, cols], preferred_element_type=F32).astype(BF)
            for i in range(first, end):
                exchange_up(g, at, i).start()

        near[2]()
        near[3]()
        normalize(0, r["x_mid"], mine, r["v_g_mlp"], layer)
        quarter = n_up // 4
        send_up(0, mine, 0, 1)
        send_up(0, mine, 1, quarter)
        send_up(0, mine, quarter, 2 * quarter)
        far[2]()
        send_up(0, mine, 2 * quarter, 3 * quarter)
        send_up(0, mine, 3 * quarter, n_up)
        far[3]()
        normalize(1, r["x_mid"], theirs, r["v_g_mlp"], layer)
        send_up(1, theirs, 0, quarter)
        send_up(1, theirs, quarter, 2 * quarter)
        send_up(1, theirs, 2 * quarter, n_up)

        if qkv:
            for c in cache_copies(0) + cache_copies(1):
                c.start()

        for g in range(2):
            sum_copy(g).wait()
        for g, at in enumerate((mine, theirs)):
            for j, f in enumerate(factors(r["ss_send"][g], r["ss_recv"][1 - g])):
                r["fac"][j, at] = jnp.broadcast_to(f, (rows, 128))

        def activate(g, at, first, end):
            for i in range(first, end):
                exchange_up(g, (mine, theirs)[g], i).wait()
            cols = slice(first * UP_CHUNK, end * UP_CHUNK)
            m = r["up_send"][at, cols].astype(F32) * r["fac"][0, at][:, 0:1] + r["up_recv"][at, cols].astype(F32) * r["fac"][1, at][:, 0:1]
            r["up_recv"][at, cols] = jax.nn.gelu(m.astype(BF).astype(F32), approximate=True).astype(BF)

        def consume(g, at, first, end):
            if g == 0:
                for i in range(first, end):
                    down_copy(i).wait()
            activate(g, at, first, end)
            span = slice(first * UP_CHUNK, end * UP_CHUNK)
            got = jnp.dot(r["up_recv"][at, span], r["wdn"][span, :], preferred_element_type=F32)
            r["acc"][at] = got if first == 0 else r["acc"][at] + got

        def last_part(cols):
            span = slice(3 * quarter * UP_CHUNK, ff)
            return r["acc"][mine, cols] + jnp.dot(r["up_recv"][mine, span], r["wdn"][span, cols], preferred_element_type=F32)

        x_now = r["x_end"]
        far = reducer(2, 1, theirs, 2, lambda cols: r["acc"][theirs, cols], r["x_mid"], r["x_end"])
        near = reducer(3, 1, mine, 2, last_part, r["x_mid"], r["x_end"])
        consume(0, theirs, 0, n_up)
        far[0]()
        consume(1, mine, 0, 2 * quarter)
        far[1]()
        consume(1, mine, 2 * quarter, 3 * quarter)
        activate(1, mine, 3 * quarter, n_up)
        near[0]()
        if not qkv:
            near[1]()
            far[2]()
            far[3]()
        else:
            near[1]()
            far[2]()
            flatten(0)
            far[3]()
            operand["g_attn"].wait()
            normalize(2, x_now, theirs, r["v_g_attn"], qkv_layer)
            send_rows(0)
            flatten(1)
            send_rows(1)
        near[2]()
        if qkv:
            flatten(2)
        near[3]()
        r["x_out"][...] = r["x_end"][...]

    if qkv:
        heads, hd = r["wraw"].shape[2:]
        if not pre:
            operand["g_attn"].wait()
            operand["hidden"].wait()
            normalize(2, x_now, theirs, r["v_g_attn"], qkv_layer)
        normalize(3, x_now, mine, r["v_g_attn"], qkv_layer, send=False)
        if pre:
            project(2, everyone, r["part"])
            r["qkv_send"][2] = r["part"][theirs].astype(BF)
            swap(2).start()
            r["qkv_own"][2] = r["part"][mine].astype(BF)
        if not pre:
            for m in range(3):
                flatten(m)
                project(m, everyone, r["part"])
                r["qkv_send"][m] = r["part"][theirs].astype(BF)
                swap(m).start()
                r["qkv_own"][m] = r["part"][mine].astype(BF)
        else:
            for m in range(2):
                project(m, mine, r["qkv_own"].at[m])
        reverse_rel()
        operand["bias_u"].wait()
        operand["bias_w"].wait()
        sum_copy(2).wait()
        own_fac, peer_fac = factors(r["ss_send"][3], r["ss_recv"][2])
        for m in range(3):
            swap(m).wait()
            full = (r["qkv_own"][m].astype(F32) * own_fac + r["qkv_recv"][m].astype(F32) * peer_fac).astype(BF).astype(F32)
            for hh in range(heads):
                head = full[:, hh * hd:(hh + 1) * hd]
                if m:
                    r[("k", "v")[m - 1]][:, hh, :] = head
                else:
                    r["a"][:, hh, :] = (head + r["v_bias_u"][qkv_layer, hh:hh + 1].astype(F32)).astype(BF).astype(F32)
                    r["c"][:, hh, :] = (head + r["v_bias_w"][qkv_layer, hh:hh + 1].astype(F32)).astype(BF).astype(F32)
        for c in cache_copies(0) + cache_copies(1):
            c.wait()


def stage(pre, qkv, layer, hidden, ctx, w):
    batch, width = hidden.shape
    heads, hd = w["w_q"].shape[2:]
    rows, half, flat = batch // 2, width // 2, heads * hd
    ff = w["w_up"].shape[2]
    n_up = ff // UP_CHUNK
    vm = pl.BlockSpec(memory_space=pltpu.VMEM)
    any_ = pl.BlockSpec(memory_space=pltpu.HBM)
    dma = pltpu.SemaphoreType.DMA
    gain = pltpu.VMEM(w["norm_mlp"].shape, BF)
    ins = [("hidden", hidden)]
    placed = {"ctx"} if layer == 0 else {"ctx", "hidden"}
    outs = []
    scratch = [("ss_send", pltpu.VMEM((4, 8, 128), F32)), ("ss_recv", pltpu.VMEM((3, 8, 128), F32)), ("ss_sem", dma((2, 3))),
               ("fac", pltpu.VMEM((2, batch, 128), F32)),
               ("h", pltpu.VMEM((batch, width), BF)), ("part", pltpu.VMEM((batch, half), F32)),
               ("op_sem", dma((6,))),
               ("wup", pltpu.VMEM((width, ff if pre else 3 * flat), BF))]
    if "hidden" not in placed:
        scratch += [("v_hidden", pltpu.VMEM((batch, width), BF))]
    if pre:
        ins += [("ctx", ctx), ("g_mlp", w["norm_mlp"]), ("w_out", w["w_out"]), ("w_up", w["w_up"]), ("w_down", w["w_down"])]
        outs += [("x_out", (batch, width), BF)]
        part = pltpu.VMEM((2, batch, half), BF)
        scratch += [("v_g_mlp", gain),
                    ("wo", pltpu.VMEM((flat, width), BF)), ("wo_sem", dma((4,))), ("wup_sem", dma((n_up,))),
                    ("wdn", pltpu.VMEM((ff, width), BF)), ("wdn_sem", dma((n_up,))),
                    ("pair_send", pltpu.VMEM((batch, half), BF)), ("pair_recv", part), ("pair_sem", dma((2, 4, 4))),
                    ("chip_send", pltpu.VMEM((batch, half), BF)), ("chip_recv", part), ("chip_sem", dma((2, 4, 4))), ("share_sem", dma((2, 4, 4))),
                    ("ctx_all", pltpu.VMEM((batch, flat), BF)), ("ctx_sem", dma((2, 1))),
                    ("x_mid", pltpu.VMEM((batch, width), BF)), ("x_end", pltpu.VMEM((batch, width), BF)),
                    ("up_send", pltpu.VMEM((batch, ff), BF)), ("up_recv", pltpu.VMEM((batch, ff), BF)), ("up_sem", dma((2, 2, n_up))),
                    ("acc", pltpu.VMEM((batch, width), F32))]
    if qkv:
        ins += [("g_attn", w["norm_attn"]), ("w_q", w["w_q"]), ("w_k", w["w_k"]), ("w_v", w["w_v"]), ("k_cache", w["k_cache"]), ("v_cache", w["v_cache"])]
        ins += [("rel", w["rel"]), ("bias_u", w["bias_u"]), ("bias_w", w["bias_w"])]
        seq = w["rel"].shape[1]
        outs += [(n, (rows, heads, hd), F32) for n in ("a", "c", "k", "v")]
        outs += [("rext", (2 * seq * heads, hd), BF)]
        outs += [(n, w["k_cache"].shape[1:], BF) for n in ("k_now", "v_now")]
        share = pltpu.VMEM((3, rows, flat), BF)
        scratch += [("v_" + n, pltpu.VMEM(w[n].shape, BF)) for n in ("bias_u", "bias_w")]
        scratch += [("v_rel", pltpu.VMEM((seq, heads, hd), BF))]
        scratch += [("v_g_attn", gain), ("cache_sem", dma((2, 4))),
                    ("wraw", pltpu.VMEM((4, 256 if pre else 512, heads, hd), BF)), ("wraw_sem", dma((4,))),
                    ("qkv_send", share), ("qkv_recv", share), ("qkv_own", share), ("qkv_sem", dma((2, 3)))]
    names = [n for n, *_ in ins] + [n for n, *_ in outs] + [n for n, _ in scratch]
    args = [pltpu.with_memory_space_constraint(a, pltpu.VMEM if n in placed else pltpu.HBM) for n, a in ins]
    return pl.pallas_call(
        functools.partial(stage_body, pre, qkv, layer, names),
        out_shape=tuple(pltpu.VMEM(s, d) if qkv else jax.ShapeDtypeStruct(s, d) for _, s, d in outs),
        in_specs=[vm if n in placed else any_ for n, _ in ins],
        out_specs=tuple(vm for _ in outs),
        scratch_shapes=[s for _, s in scratch],
        compiler_params=pltpu.CompilerParams(collective_id=(1 if pre else 0) + (2 if qkv else 0), has_side_effects=True, vmem_limit_bytes=VMEM_LIMIT),
        name=f"stage_{int(pre)}{int(qkv)}",
    )(*args)


def solution(mesh):
    cache_spec = P(None, ("rep", "y"), None, "x", None)
    row_spec = P("rep", "y")
    proj_spec = P(None, "y", "x", None)
    head_spec = P(None, "x", None)
    in_specs = (row_spec, P("rep"), cache_spec, cache_spec, P(None, None, "x", None), P(None, "y"),
                proj_spec, proj_spec, proj_spec, head_spec, head_spec, P(None, "x", None, "y"),
                P(None, "y"), P(None, "y", "x"), P(None, "x", "y"))
    out_specs = (row_spec, cache_spec, cache_spec)

    def local_step(hidden, lengths, k_cache, v_cache, rel_table, norm_attn, w_q, w_k, w_v, bias_content, bias_pos, w_out, norm_mlp, w_up, w_down):
        layers, rows, seq, heads, hd = k_cache.shape
        merged = (layers, rows, seq * heads, hd)
        w = dict(norm_attn=norm_attn, w_q=w_q, w_k=w_k, w_v=w_v, norm_mlp=norm_mlp, w_up=w_up, w_down=w_down,
                 w_out=w_out.reshape(w_out.shape[0], -1, w_out.shape[3]), k_cache=k_cache.reshape(merged), v_cache=v_cache.reshape(merged),
                 rel=rel_table, bias_u=bias_content, bias_w=bias_pos)
        fed = stage(False, True, 0, hidden, None, w)
        prev = None
        for layer in range(layers):
            ctx, *prev = attend_cache(layer, lengths, fed, layers, prev)
            if layer + 1 < layers:
                hidden, *fed = stage(True, True, layer, hidden, ctx, w)
            else:
                hidden, = stage(True, False, layer, hidden, ctx, w)
        return hidden, prev[0].reshape(k_cache.shape), prev[1].reshape(v_cache.shape)

    return jax.shard_map(local_step, mesh=mesh, in_specs=in_specs, out_specs=out_specs, check_vma=False)
```

```python
import functools
import jax
import jax.numpy as jnp
from jax import lax
from jax.experimental import pallas as pl
from jax.experimental.pallas import tpu as pltpu
from jax.sharding import PartitionSpec as P

BF = jnp.bfloat16
F32 = jnp.float32

def attn_body(layer, group, len_ref, a_ref, c_ref, kn_ref, vn_ref, rext, k_in, v_in, *rest):
    ctx_ref, ko, vo, kbuf, vbuf, wsem = rest[-6:]
    rows, span, hd = kbuf.shape
    heads = a_ref.shape[1]
    seq = span // heads
    y = lax.axis_index("y")
    n_grp = rows // group

    @pl.loop(0, rows, unroll=4)
    def _(b):
        at = pl.ds(pl.multiple_of(len_ref[y * rows + b] * heads, heads), heads)
        kbuf[b, at] = kn_ref[b].astype(BF)
        vbuf[b, at] = vn_ref[b].astype(BF)

    col = lax.broadcasted_iota(jnp.int32, (heads, span), 1)
    row = lax.broadcasted_iota(jnp.int32, (heads, span), 0)
    own = (col % heads) == row
    pos = jnp.where(own, col // heads, 1 << 20)
    scale = hd ** -0.5

    def save(i):
        sl = pl.ds(i * group, group)
        return (pltpu.make_async_copy(kbuf.at[sl], ko.at[layer, sl], wsem.at[0, i]),
                pltpu.make_async_copy(vbuf.at[sl], vo.at[layer, sl], wsem.at[1, i]))

    @pl.loop(0, n_grp)
    def _(i):
        for c in save(i):
            c.start()

    @pl.loop(0, n_grp)
    def _(i):
        score = []
        for g in range(group):
            b = i * group + g
            ln = len_ref[y * rows + b]
            rr = rext[pl.ds(pl.multiple_of((seq - 1 - ln) * heads, heads), span)]
            lhs = jnp.concatenate([a_ref[b].astype(BF), c_ref[b].astype(BF)], axis=1)
            rhs = jnp.concatenate([kbuf[b], rr], axis=1)
            s = lax.dot_general(lhs, rhs, (((1,), (1,)), ((), ())), preferred_element_type=F32)
            score.append(jnp.where(pos <= ln, s * scale, -1e30))
        prob = []
        for g in range(group):
            s = score[g]
            m = jnp.max(s, axis=1, keepdims=True)
            e = jnp.exp(s - m)
            prob.append((e / jnp.sum(e, axis=1, keepdims=True)).astype(BF))
        for g in range(group):
            b = i * group + g
            o = jnp.dot(prob[g], vbuf[b], preferred_element_type=F32)
            ctx_ref[b] = o.astype(BF).astype(F32)

    @pl.loop(0, n_grp)
    def _(i):
        for c in save(i):
            c.wait()


def attend_cache(layer, lengths, fed, layers, prev, group=16):
    rows, span, hd = fed[-1].shape
    heads = fed[0].shape[1]
    any_ = pl.BlockSpec(memory_space=pltpu.HBM)
    vm = pl.BlockSpec(memory_space=pltpu.VMEM)
    n_grp = rows // group
    ins = [lengths] + [pltpu.with_memory_space_constraint(c, pltpu.VMEM) for c in fed]
    specs = [pl.BlockSpec(memory_space=pltpu.SMEM)] + [vm] * len(fed)
    alias = {6: 3, 7: 4}
    if prev is not None:
        ins += prev
        specs += [any_, any_]
        alias.update({8: 1, 9: 2})
    cache = jax.ShapeDtypeStruct((layers, rows, span, hd), BF)
    now = jax.ShapeDtypeStruct(fed[-1].shape, BF)
    return pl.pallas_call(
        functools.partial(attn_body, layer, group),
        out_shape=(pltpu.VMEM((rows, heads, hd), F32), cache, cache, now, now),
        in_specs=specs, out_specs=(vm, any_, any_, vm, vm), input_output_aliases=alias,
        scratch_shapes=[pltpu.SemaphoreType.DMA((2, n_grp))],
        compiler_params=pltpu.CompilerParams(vmem_limit_bytes=24 << 20),
        name=f"attend_{layer}")(*ins)[:3]


MESH = pl.DeviceIdType.MESH
EPS = 1e-6
UP_CHUNK = 512
VMEM_LIMIT = 46399488


def rows_to_cols(col):
    square = jnp.concatenate([col] * (128 // col.shape[0]), axis=0)
    return jnp.broadcast_to(jnp.sum(square.T, axis=0, keepdims=True), (8, 128))


def cols_to_rows(row, n):
    return jnp.broadcast_to(row[0:1], (128, 128)).T[:n, 0:1]


def stage_body(pre, qkv, layer, names, *refs):
    r = dict(zip(names, refs))
    batch, width = r["h"].shape
    ops = [n[2:] for n in names if n.startswith("v_") and n[2:] in names]
    operand = {n: pltpu.make_async_copy(r[n] if n != "rel" else r[n].at[layer + int(pre)], r["v_" + n], r["op_sem"].at[i]) for i, n in enumerate(ops)}
    for n in ops:
        operand[n].start()
    half = width // 2
    rows = batch // 2
    x = lax.axis_index("x")
    y = lax.axis_index("y")
    y_dev = {"y": 1 - y}
    core = x % 2
    pair_dev = {"x": x + 1 - 2 * core}
    mine = pl.ds(pl.multiple_of(y * rows, rows), rows)
    theirs = pl.ds(pl.multiple_of((1 - y) * rows, rows), rows)
    everyone = pl.ds(0, batch)
    chip_dev = {"x": (x + 2) % 4}
    qkv_layer = layer + 1 if pre else layer

    def remote(src, dst, sems, idx, dev):
        return pltpu.make_async_remote_copy(src, dst, r[sems].at[0, idx], r[sems].at[1, idx], device_id=dev, device_id_type=MESH)

    def wo_copy(i):
        n = r["wo"].shape[0] // 4
        return pltpu.make_async_copy(r["w_out"].at[layer, pl.ds(i * n, n)], r["wo"].at[pl.ds(i * n, n)], r["wo_sem"].at[i])

    def up_copy(i):
        cols = pl.ds(pl.multiple_of(i * UP_CHUNK, UP_CHUNK), UP_CHUNK)
        return pltpu.make_async_copy(r["w_up"].at[layer, :, cols], r["wup"].at[:, cols], r["wup_sem"].at[i])

    def down_copy(i):
        sl = pl.ds(i * UP_CHUNK, UP_CHUNK)
        return pltpu.make_async_copy(r["w_down"].at[layer, sl], r["wdn"].at[sl], r["wdn_sem"].at[i])

    slots, raw_rows = r["wraw"].shape[:2] if qkv else (1, width)
    turns = width // (slots * raw_rows)

    def cache_copies(i):
        src, dst = (("k_cache", "k_now"), ("v_cache", "v_now"))[i]
        n = r[dst].shape[0] // 4
        return [pltpu.make_async_copy(r[src].at[qkv_layer, pl.ds(j * n, n)], r[dst].at[pl.ds(j * n, n)], r["cache_sem"].at[i, j]) for j in range(4)]

    def raw_copy(m, turn, j):
        sl = pl.ds((turn * slots + j) * raw_rows, raw_rows)
        return pltpu.make_async_copy(r[("w_q", "w_k", "w_v")[m]].at[qkv_layer, sl], r["wraw"].at[j], r["wraw_sem"].at[j])

    def start_qkv():
        for j in range(slots):
            raw_copy(0, 0, j).start()

    def flatten(m):
        heads, hd = r["wraw"].shape[2:]
        for turn in range(turns):
            after = (m, turn + 1) if turn + 1 < turns else (m + 1, 0)

            @pl.loop(0, slots)
            def _(j):
                raw_copy(m, turn, j).wait()

                @pl.loop(0, raw_rows // 256)
                def _(b):
                    off = pl.multiple_of(b * 256, 256)
                    by_head = jnp.swapaxes(r["wraw"][j, pl.ds(off, 256)], 0, 1)
                    sl = pl.ds(pl.multiple_of((turn * slots + j) * raw_rows + off, 256), 256)
                    for hh in range(heads):
                        col = m * heads * hd + hh * hd
                        r["wup"][sl, col:col + hd] = by_head[hh]

                if after[0] < 3:
                    raw_copy(*after, j).start()

        if m < 2 and not pre:
            for c in cache_copies(m):
                c.start()

    def project(m, at, dst):
        lanes = dst.shape[1]
        for j in range(lanes // 256):
            cols = slice(j * 256, (j + 1) * 256)
            dst[:, cols] = jnp.dot(r["h"][at], r["wup"][:, m * lanes + j * 256:m * lanes + (j + 1) * 256], preferred_element_type=F32).astype(dst.dtype)

    def swap(m):
        return remote(r["qkv_send"].at[m], r["qkv_recv"].at[m], "qkv_sem", m, y_dev)

    def send_rows(m):
        project(m, theirs, r["qkv_send"].at[m])
        swap(m).start()

    def reverse_rel():
        operand["rel"].wait()
        seq, heads, hd = r["v_rel"].shape

        @pl.loop(0, seq, unroll=4)
        def _(t):
            r["rext"][pl.ds(pl.multiple_of((seq - 1 - t) * heads, heads), heads)] = r["v_rel"][t]
            r["rext"][pl.ds(pl.multiple_of((seq + t) * heads, heads), heads)] = jnp.zeros((heads, hd), BF)

    if pre:
        n_up = r["wup"].shape[1] // UP_CHUNK
        for i in range(4):
            wo_copy(i).start()

        @pl.loop(0, n_up)
        def _(i):
            up_copy(i).start()
    else:
        start_qkv()

    barrier = pltpu.get_barrier_semaphore()
    greet = [y_dev, pair_dev, chip_dev] if pre else [y_dev]
    for dev in greet:
        pl.semaphore_signal(barrier, inc=1, device_id=dev, device_id_type=MESH)
    pl.semaphore_wait(barrier, len(greet))

    def row_sums(wide):
        sq = wide * wide
        part = sq[:, 0:128]
        for j in range(1, wide.shape[1] // 128):
            part = part + sq[:, j * 128:(j + 1) * 128]
        return part

    def sum_copy(slot):
        return remote(r["ss_send"].at[slot], r["ss_recv"].at[slot], "ss_sem", slot, y_dev)

    def inv_rms(sums):
        return lax.rsqrt(cols_to_rows(sums, rows) / (2 * width) + EPS)

    def normalize(slot, x_ref, at, gain_ref, gain_layer, send=True):
        wide = x_ref[at].astype(F32)
        r["ss_send"][slot] = rows_to_cols(row_sums(wide))
        if send:
            sum_copy(slot).start()
        gain = gain_ref[pl.ds(gain_layer, 1)].astype(F32)
        r["h"][at] = (x_ref[at].astype(F32) * inv_rms(r["ss_send"][slot]) * gain).astype(BF)

    def factors(own_sums, peer_sums):
        whole = inv_rms(own_sums + peer_sums)
        return whole / jnp.maximum(inv_rms(own_sums), 1e-30), whole / jnp.maximum(inv_rms(peer_sums), 1e-30)

    def half_of(side):
        return pl.ds(pl.multiple_of(side * half, half), half)

    def reducer(slot, bank, at, pieces, part_of, x_ref, out_ref):
        step = half // pieces

        def copy(kind, c=0):
            here = pl.ds(c * step, step) if kind == "chip" else pl.ds(0, half)
            if kind == "share":
                src = dst = out_ref.at[at, pl.ds(pl.multiple_of(core * half + c * step, step), step)]
            else:
                src, dst = r[kind + "_send"].at[at, here], r[kind + "_recv"].at[bank, at, here]
            sems = r[kind + "_sem"]
            return pltpu.make_async_remote_copy(src, dst, sems.at[0, slot, c], sems.at[1, slot, c],
                                                device_id=chip_dev if kind == "chip" else pair_dev, device_id_type=MESH)

        def begin():
            r["pair_send"][at] = part_of(half_of(1 - core)).astype(BF)
            copy("pair").start()
            r["part"][at] = part_of(half_of(core))

        def cross():
            copy("pair").wait()
            for c in range(pieces):
                here = slice(c * step, (c + 1) * step)
                r["chip_send"][at, here] = (r["part"][at, here] + r["pair_recv"][bank, at, here].astype(F32)).astype(BF)
                copy("chip", c).start()

        def land():
            for c in range(pieces):
                copy("chip", c).wait()
                here = slice(c * step, (c + 1) * step)
                cols = pl.ds(pl.multiple_of(core * half + c * step, step), step)
                total = r["chip_send"][at, here].astype(F32) + r["chip_recv"][bank, at, here].astype(F32)
                out_ref[at, cols] = (x_ref[at, cols].astype(F32) + total).astype(BF)
                copy("share", c).start()

        def finish():
            for c in range(pieces):
                copy("share", c).wait()

        return begin, cross, land, finish

    x_now = r["v_hidden"] if "hidden" in ops else r["hidden"]
    if pre:
        heads, hd = r["ctx"].shape[1:]
        for hh in range(heads):
            r["ctx_all"][mine, hh * hd:(hh + 1) * hd] = r["ctx"][:, hh, :].astype(BF)
        ctx_copy = remote(r["ctx_all"].at[mine], r["ctx_all"].at[mine], "ctx_sem", 0, y_dev)
        ctx_copy.start()

        def wo_part(at):
            return lambda cols: jnp.dot(r["ctx_all"][at], r["wo"][:, cols], preferred_element_type=F32)

        near = reducer(0, 0, mine, 2, wo_part(mine), x_now, r["x_mid"])
        far = reducer(1, 0, theirs, 2, wo_part(theirs), x_now, r["x_mid"])
        for i in range(4):
            wo_copy(i).wait()
        near[0]()
        near[1]()

        @pl.loop(0, n_up)
        def _(i):
            down_copy(i).start()
        if qkv:
            start_qkv()
        ctx_copy.wait()
        far[0]()
        far[1]()
        if "hidden" in ops:
            operand["hidden"].wait()
        operand["g_mlp"].wait()

        ff = r["wup"].shape[1]

        def exchange_up(g, at, i):
            cols = pl.ds(i * UP_CHUNK, UP_CHUNK)
            return pltpu.make_async_remote_copy(r["up_send"].at[at, cols], r["up_recv"].at[at, cols], r["up_sem"].at[0, g, i], r["up_sem"].at[1, g, i],
                                                device_id=y_dev, device_id_type=MESH)

        def send_up(g, at, first, end):
            cols = slice(first * UP_CHUNK, end * UP_CHUNK)
            if g == 0:
                for i in range(first, end):
                    up_copy(i).wait()
            r["up_send"][at, cols] = jnp.dot(r["h"][at], r["wup"][:, cols], preferred_element_type=F32).astype(BF)
            for i in range(first, end):
                exchange_up(g, at, i).start()

        near[2]()
        near[3]()
        normalize(0, r["x_mid"], mine, r["v_g_mlp"], layer)
        quarter = n_up // 4
        send_up(0, mine, 0, 1)
        send_up(0, mine, 1, quarter)
        send_up(0, mine, quarter, 2 * quarter)
        far[2]()
        send_up(0, mine, 2 * quarter, 3 * quarter)
        send_up(0, mine, 3 * quarter, n_up)
        far[3]()
        normalize(1, r["x_mid"], theirs, r["v_g_mlp"], layer)
        send_up(1, theirs, 0, quarter)
        send_up(1, theirs, quarter, 2 * quarter)
        send_up(1, theirs, 2 * quarter, n_up)

        if qkv:
            for c in cache_copies(0) + cache_copies(1):
                c.start()

        for g in range(2):
            sum_copy(g).wait()
        for g, at in enumerate((mine, theirs)):
            for j, f in enumerate(factors(r["ss_send"][g], r["ss_recv"][1 - g])):
                r["fac"][j, at] = jnp.broadcast_to(f, (rows, 128))

        def activate(g, at, first, end):
            for i in range(first, end):
                exchange_up(g, (mine, theirs)[g], i).wait()
            cols = slice(first * UP_CHUNK, end * UP_CHUNK)
            m = r["up_send"][at, cols].astype(F32) * r["fac"][0, at][:, 0:1] + r["up_recv"][at, cols].astype(F32) * r["fac"][1, at][:, 0:1]
            r["up_recv"][at, cols] = jax.nn.gelu(m.astype(BF).astype(F32), approximate=True).astype(BF)

        def consume(g, at, first, end):
            if g == 0:
                for i in range(first, end):
                    down_copy(i).wait()
            activate(g, at, first, end)
            span = slice(first * UP_CHUNK, end * UP_CHUNK)
            got = jnp.dot(r["up_recv"][at, span], r["wdn"][span, :], preferred_element_type=F32)
            r["acc"][at] = got if first == 0 else r["acc"][at] + got

        def last_part(cols):
            span = slice(3 * quarter * UP_CHUNK, ff)
            return r["acc"][mine, cols] + jnp.dot(r["up_recv"][mine, span], r["wdn"][span, cols], preferred_element_type=F32)

        x_now = r["x_end"]
        far = reducer(2, 1, theirs, 2, lambda cols: r["acc"][theirs, cols], r["x_mid"], r["x_end"])
        near = reducer(3, 1, mine, 2, last_part, r["x_mid"], r["x_end"])
        consume(0, theirs, 0, n_up)
        far[0]()
        consume(1, mine, 0, 2 * quarter)
        far[1]()
        consume(1, mine, 2 * quarter, 3 * quarter)
        activate(1, mine, 3 * quarter, n_up)
        near[0]()
        if not qkv:
            near[1]()
            far[2]()
            far[3]()
        else:
            near[1]()
            far[2]()
            flatten(0)
            far[3]()
            operand["g_attn"].wait()
            normalize(2, x_now, theirs, r["v_g_attn"], qkv_layer)
            send_rows(0)
            flatten(1)
            send_rows(1)
        near[2]()
        if qkv:
            flatten(2)
        near[3]()
        r["x_out"][...] = r["x_end"][...]

    if qkv:
        heads, hd = r["wraw"].shape[2:]
        if not pre:
            operand["g_attn"].wait()
            operand["hidden"].wait()
            normalize(2, x_now, theirs, r["v_g_attn"], qkv_layer)
        normalize(3, x_now, mine, r["v_g_attn"], qkv_layer, send=False)
        if pre:
            project(2, everyone, r["part"])
            r["qkv_send"][2] = r["part"][theirs].astype(BF)
            swap(2).start()
            r["qkv_own"][2] = r["part"][mine].astype(BF)
        if not pre:
            for m in range(3):
                flatten(m)
                project(m, everyone, r["part"])
                r["qkv_send"][m] = r["part"][theirs].astype(BF)
                swap(m).start()
                r["qkv_own"][m] = r["part"][mine].astype(BF)
        else:
            for m in range(2):
                project(m, mine, r["qkv_own"].at[m])
        reverse_rel()
        operand["bias_u"].wait()
        operand["bias_w"].wait()
        sum_copy(2).wait()
        own_fac, peer_fac = factors(r["ss_send"][3], r["ss_recv"][2])
        for m in range(3):
            swap(m).wait()
            full = (r["qkv_own"][m].astype(F32) * own_fac + r["qkv_recv"][m].astype(F32) * peer_fac).astype(BF).astype(F32)
            for hh in range(heads):
                head = full[:, hh * hd:(hh + 1) * hd]
                if m:
                    r[("k", "v")[m - 1]][:, hh, :] = head
                else:
                    r["a"][:, hh, :] = (head + r["v_bias_u"][qkv_layer, hh:hh + 1].astype(F32)).astype(BF).astype(F32)
                    r["c"][:, hh, :] = (head + r["v_bias_w"][qkv_layer, hh:hh + 1].astype(F32)).astype(BF).astype(F32)
        for c in cache_copies(0) + cache_copies(1):
            c.wait()


def stage(pre, qkv, layer, hidden, ctx, w):
    batch, width = hidden.shape
    heads, hd = w["w_q"].shape[2:]
    rows, half, flat = batch // 2, width // 2, heads * hd
    ff = w["w_up"].shape[2]
    n_up = ff // UP_CHUNK
    vm = pl.BlockSpec(memory_space=pltpu.VMEM)
    any_ = pl.BlockSpec(memory_space=pltpu.HBM)
    dma = pltpu.SemaphoreType.DMA
    gain = pltpu.VMEM(w["norm_mlp"].shape, BF)
    ins = [("hidden", hidden)]
    placed = {"ctx"} if layer == 0 else {"ctx", "hidden"}
    outs = []
    scratch = [("ss_send", pltpu.VMEM((4, 8, 128), F32)), ("ss_recv", pltpu.VMEM((3, 8, 128), F32)), ("ss_sem", dma((2, 3))),
               ("fac", pltpu.VMEM((2, batch, 128), F32)),
               ("h", pltpu.VMEM((batch, width), BF)), ("part", pltpu.VMEM((batch, half), F32)),
               ("op_sem", dma((6,))),
               ("wup", pltpu.VMEM((width, ff if pre else 3 * flat), BF))]
    if "hidden" not in placed:
        scratch += [("v_hidden", pltpu.VMEM((batch, width), BF))]
    if pre:
        ins += [("ctx", ctx), ("g_mlp", w["norm_mlp"]), ("w_out", w["w_out"]), ("w_up", w["w_up"]), ("w_down", w["w_down"])]
        outs += [("x_out", (batch, width), BF)]
        part = pltpu.VMEM((2, batch, half), BF)
        scratch += [("v_g_mlp", gain),
                    ("wo", pltpu.VMEM((flat, width), BF)), ("wo_sem", dma((4,))), ("wup_sem", dma((n_up,))),
                    ("wdn", pltpu.VMEM((ff, width), BF)), ("wdn_sem", dma((n_up,))),
                    ("pair_send", pltpu.VMEM((batch, half), BF)), ("pair_recv", part), ("pair_sem", dma((2, 4, 4))),
                    ("chip_send", pltpu.VMEM((batch, half), BF)), ("chip_recv", part), ("chip_sem", dma((2, 4, 4))), ("share_sem", dma((2, 4, 4))),
                    ("ctx_all", pltpu.VMEM((batch, flat), BF)), ("ctx_sem", dma((2, 1))),
                    ("x_mid", pltpu.VMEM((batch, width), BF)), ("x_end", pltpu.VMEM((batch, width), BF)),
                    ("up_send", pltpu.VMEM((batch, ff), BF)), ("up_recv", pltpu.VMEM((batch, ff), BF)), ("up_sem", dma((2, 2, n_up))),
                    ("acc", pltpu.VMEM((batch, width), F32))]
    if qkv:
        ins += [("g_attn", w["norm_attn"]), ("w_q", w["w_q"]), ("w_k", w["w_k"]), ("w_v", w["w_v"]), ("k_cache", w["k_cache"]), ("v_cache", w["v_cache"])]
        ins += [("rel", w["rel"]), ("bias_u", w["bias_u"]), ("bias_w", w["bias_w"])]
        seq = w["rel"].shape[1]
        outs += [(n, (rows, heads, hd), F32) for n in ("a", "c", "k", "v")]
        outs += [("rext", (2 * seq * heads, hd), BF)]
        outs += [(n, w["k_cache"].shape[1:], BF) for n in ("k_now", "v_now")]
        share = pltpu.VMEM((3, rows, flat), BF)
        scratch += [("v_" + n, pltpu.VMEM(w[n].shape, BF)) for n in ("bias_u", "bias_w")]
        scratch += [("v_rel", pltpu.VMEM((seq, heads, hd), BF))]
        scratch += [("v_g_attn", gain), ("cache_sem", dma((2, 4))),
                    ("wraw", pltpu.VMEM((4, 256 if pre else 512, heads, hd), BF)), ("wraw_sem", dma((4,))),
                    ("qkv_send", share), ("qkv_recv", share), ("qkv_own", share), ("qkv_sem", dma((2, 3)))]
    names = [n for n, *_ in ins] + [n for n, *_ in outs] + [n for n, _ in scratch]
    args = [pltpu.with_memory_space_constraint(a, pltpu.VMEM if n in placed else pltpu.HBM) for n, a in ins]
    return pl.pallas_call(
        functools.partial(stage_body, pre, qkv, layer, names),
        out_shape=tuple(pltpu.VMEM(s, d) if qkv else jax.ShapeDtypeStruct(s, d) for _, s, d in outs),
        in_specs=[vm if n in placed else any_ for n, _ in ins],
        out_specs=tuple(vm for _ in outs),
        scratch_shapes=[s for _, s in scratch],
        compiler_params=pltpu.CompilerParams(collective_id=(1 if pre else 0) + (2 if qkv else 0), has_side_effects=True, vmem_limit_bytes=VMEM_LIMIT),
        name=f"stage_{int(pre)}{int(qkv)}",
    )(*args)


def solution(mesh):
    cache_spec = P(None, ("rep", "y"), None, "x", None)
    row_spec = P("rep", "y")
    proj_spec = P(None, "y", "x", None)
    head_spec = P(None, "x", None)
    in_specs = (row_spec, P("rep"), cache_spec, cache_spec, P(None, None, "x", None), P(None, "y"),
                proj_spec, proj_spec, proj_spec, head_spec, head_spec, P(None, "x", None, "y"),
                P(None, "y"), P(None, "y", "x"), P(None, "x", "y"))
    out_specs = (row_spec, cache_spec, cache_spec)

    def local_step(hidden, lengths, k_cache, v_cache, rel_table, norm_attn, w_q, w_k, w_v, bias_content, bias_pos, w_out, norm_mlp, w_up, w_down):
        layers, rows, seq, heads, hd = k_cache.shape
        merged = (layers, rows, seq * heads, hd)
        w = dict(norm_attn=norm_attn, w_q=w_q, w_k=w_k, w_v=w_v, norm_mlp=norm_mlp, w_up=w_up, w_down=w_down,
                 w_out=w_out.reshape(w_out.shape[0], -1, w_out.shape[3]), k_cache=k_cache.reshape(merged), v_cache=v_cache.reshape(merged),
                 rel=rel_table, bias_u=bias_content, bias_w=bias_pos)
        fed = stage(False, True, 0, hidden, None, w)
        prev = None
        for layer in range(layers):
            ctx, *prev = attend_cache(layer, lengths, fed, layers, prev)
            if layer + 1 < layers:
                hidden, *fed = stage(True, True, layer, hidden, ctx, w)
            else:
                hidden, = stage(True, False, layer, hidden, ctx, w)
        return hidden, prev[0].reshape(k_cache.shape), prev[1].reshape(v_cache.shape)

    return jax.shard_map(local_step, mesh=mesh, in_specs=in_specs, out_specs=out_specs, check_vma=False)
```
